128 devices in a mesh: dp: 1, cols: 16 (over z, y), rows: 8 (over x, core).
Axes of the slice: x: 4, y: 4, z: 4, core: 2. Of those that a mesh axis runs over, the one named last changes fastest.
Arguments:
- h_init: bfloat16 [2, 96, 192, 384], P('dp', 'rows', 'cols')
- c_init: float32 [2, 96, 192, 384], P('dp', 'rows', 'cols')
- w_rec: bfloat16 [3, 3, 384, 1536], replicated
- gate_bias: float32 [12, 1536], replicated
Outputs:
- output 1: bfloat16 [12, 2, 96, 192, 384], P(None, 'dp', 'rows', 'cols')
- output 2: float32 [2, 96, 192, 384], P('dp', 'rows', 'cols')
All inputs are finite; a program needn't handle non-finite values.
Results may differ from the reference program's by a relative error of at most 0.00284197.
Values are sent between devices in bfloat16 or wider.
A program may use at most 1 GiB of HBM per device.

```python
import jax
import jax.numpy as jnp
from jax import lax

STEPS = 12
BATCH = 2
GRID_H = 96
GRID_W = 192
CHANNELS = 384


def setup_inputs(seed: int = 0, part: int = 0) -> dict:
    key_w, key_b = jax.random.split(jax.random.key(seed))
    part_key = jax.random.fold_in(jax.random.key(seed + 1), part)
    key_h, key_c = jax.random.split(part_key)
    fan_in = 9 * CHANNELS
    w_rec = (jax.random.normal(key_w, (3, 3, CHANNELS, 4 * CHANNELS), jnp.float32) * (1.5 * fan_in ** -0.5)).astype(jnp.bfloat16)
    gate_offset = jnp.repeat(jnp.array([0.0, 1.0, 0.0, 0.0], jnp.float32), CHANNELS)
    gate_bias = jax.random.normal(key_b, (STEPS, 4 * CHANNELS), jnp.float32) * 0.5 + gate_offset
    h_init = (jax.random.normal(key_h, (BATCH, GRID_H, GRID_W, CHANNELS), jnp.float32) * 0.6).astype(jnp.bfloat16)
    c_init = jax.random.normal(key_c, (BATCH, GRID_H, GRID_W, CHANNELS), jnp.float32)
    return {"h_init": h_init, "c_init": c_init, "w_rec": w_rec, "gate_bias": gate_bias}


def reference(h_init, c_init, w_rec, gate_bias):
    w_wide = w_rec.astype(jnp.float32)

    def one_step(carry_in, bias_row):
        h_prev, c_prev = carry_in
        gate_pre = lax.conv_general_dilated(h_prev.astype(jnp.float32), w_wide, (1, 1), "SAME", dimension_numbers=("NHWC", "HWIO", "NHWC")) + bias_row
        in_gate, forget_gate, out_gate, cand_gate = jnp.split(gate_pre, 4, axis=-1)
        c_next = jax.nn.sigmoid(forget_gate) * c_prev + jax.nn.sigmoid(in_gate) * jnp.tanh(cand_gate)
        h_next = (jax.nn.sigmoid(out_gate) * jnp.tanh(c_next)).astype(jnp.bfloat16)
        return (h_next, c_next), h_next

    final_state, h_seq = lax.scan(one_step, (h_init, c_init), gate_bias)
    return h_seq, final_state[1]
```

```python
import functools

import jax
import jax.numpy as jnp
from jax import lax
from jax.experimental import pallas as pl
from jax.experimental.pallas import tpu as pltpu
from jax.sharding import PartitionSpec as P

MESH = pl.DeviceIdType.MESH
STEPS = 12
S = 2
T = 12
LANES = 128
CH = 3
CDIM = CH * LANES
TAPS = 9
PITCH = 16
GROWS = 20 * PITCH
SLOTS = 4

DIRS = ((-1, 0), (1, 0), (0, -1), (0, 1), (-1, -1), (-1, 1), (1, -1), (1, 1))


def opposite(d):
    dy, dx = DIRS[d]
    return DIRS.index((-dy, -dx))


def at(y, x):
    return (y + 2) * PITCH + x + 2


def sigmoid(v):
    return 0.5 * jnp.tanh(0.5 * v) + 0.5


def lstm(gates, c_prev):
    i, f, o, g = (gates[:, k * LANES : (k + 1) * LANES] for k in range(4))
    c = sigmoid(f) * c_prev + sigmoid(i) * jnp.tanh(g)
    h = (sigmoid(o) * jnp.tanh(c)).astype(jnp.bfloat16)
    return h, c


def gather_tile(grid, ty, tx):
    low = lax.broadcasted_iota(jnp.int32, (8, LANES), 0) < 4
    halves = []
    for jy in (0, 2):
        a = grid[pl.ds(at(ty + 3 * jy, tx), 8, stride=3), :]
        b = grid[pl.ds(at(ty + 3 * jy + 3, tx) - 12, 8, stride=3), :]
        halves.append(jnp.where(low, a, b))
    return jnp.concatenate(halves, axis=0)


def scatter_tile(grid, ty, tx, v):
    for jy in range(4):
        grid[pl.ds(at(ty + 3 * jy, tx), 4, stride=3), :] = v[4 * jy : 4 * jy + 4]


def line(grid, y, x, n, vertical):
    return grid.at[pl.ds(at(y, x), n, stride=PITCH) if vertical else pl.ds(at(y, x), n), :]


def each(n, body):
    def step(k, carry):
        body(k)
        return carry

    lax.fori_loop(0, n, step, 0)


def sample_chunk(k):
    return lax.div(k, CH), lax.rem(k, CH)


SIDES = ((-1, -1, False), (T, -1, False), (0, -1, True), (0, T, True))
SIDE_LEN = (T + 2, T + 2, T, T)


def kernel(
    h_init, c_init, w_hbm, bias, h_seq, c_last,
    w, pt, grid, cgrid, c_own, c_ring, lhs_ring, out_st, h_own, h_ring,
    send_e, send_k, recv_e, recv_k, init_e, init_c, init_k, got_e, got_c, got_k, stage,
    w_sem, out_sem, send_sem, recv_sem, isend_sem, irecv_sem,
):
    rows_n, cols_n = lax.axis_size("rows"), lax.axis_size("cols")
    my_row, my_col = lax.axis_index("rows"), lax.axis_index("cols")

    def exists(d):
        dy, dx = DIRS[d]
        tests = []
        if dy < 0:
            tests.append(my_row > 0)
        if dy > 0:
            tests.append(my_row < rows_n - 1)
        if dx < 0:
            tests.append(my_col > 0)
        if dx > 0:
            tests.append(my_col < cols_n - 1)
        return functools.reduce(jnp.logical_and, tests)

    def peer(d):
        dy, dx = DIRS[d]
        return {"rows": my_row + dy, "cols": my_col + dx}

    for c in range(CH):
        for g in range(4):
            pltpu.make_async_copy(
                w_hbm.at[:, :, :, pl.ds(g * CDIM + c * LANES, LANES)],
                w.at[c, :, :, :, pl.ds(g * LANES, LANES)],
                w_sem.at[c],
            ).start()

    barrier = pltpu.get_barrier_semaphore()
    near = jnp.int32(0)
    for d in range(8):
        near = near + exists(d).astype(jnp.int32)

        @pl.when(exists(d))
        def _():
            pl.semaphore_signal(barrier, inc=1, device_id=peer(d), device_id_type=MESH)

    @functools.partial(each, S * CH)
    def _(k):
        s, c = sample_chunk(k)
        zero = jnp.zeros((GROWS, LANES), jnp.float32)
        grid[0, s, c] = zero
        grid[1, s, c] = zero
        cgrid[s, c] = zero

    @functools.partial(each, S * T)
    def _(k):
        s, y = lax.div(k, T), lax.rem(k, T)
        for c in range(CH):
            lanes = slice(c * LANES, (c + 1) * LANES)
            grid[0, s, c, pl.ds(at(y, 0), T), :] = h_init[s, y, :, lanes].astype(jnp.float32)
            cgrid[s, c, pl.ds(at(y, 0), T), :] = c_init[s, y, :, lanes]

    def edge_line(g, d, depth):
        dy, dx = DIRS[d]
        if dx == 0:
            return line(g, depth if dy < 0 else T - 1 - depth, 0, 16, False)
        return line(g, 0, depth if dx < 0 else T - 1 - depth, 16, True)

    def pack_messages(q, c, b):
        @functools.partial(each, S)
        def _(s):
            for d in range(4):
                send_e[b, d, c, s] = edge_line(grid.at[q, s, c], d, 1)[...].astype(jnp.bfloat16)

        @functools.partial(each, 4)
        def _(k):
            start = at(lax.div(k, 2) * (T - 2), lax.rem(k, 2) * (T - 2))
            for s in range(S):
                stage[k, pl.ds(4 * s, 2), :] = grid[q, s, c, pl.ds(start, 2), :]
                stage[k, pl.ds(4 * s + 2, 2), :] = grid[q, s, c, pl.ds(start + PITCH, 2), :]
            send_k[b, k, c] = stage[k].astype(jnp.bfloat16)

    def message(d, b, slot, sending, c=None):
        e = opposite(d) if sending else d
        if d < 4:
            src, dst = send_e.at[b, d], recv_e.at[slot, e]
        else:
            src, dst = send_k.at[b, d - 4], recv_k.at[slot, e - 4]
        if c is not None:
            src, dst = src.at[c], dst.at[c]
        return pltpu.make_async_remote_copy(
            src_ref=src, dst_ref=dst,
            send_sem=send_sem.at[b, d], recv_sem=recv_sem.at[slot, e],
            device_id=peer(d), device_id_type=MESH,
        )

    def start_messages(c, b, slot):
        for d in range(8):

            @pl.when(exists(d))
            def _():
                message(d, b, slot, True, c).start()

    def take_messages(q, b, slot):
        for d in range(8):

            @pl.when(exists(d))
            def _():
                dy, dx = DIRS[d]
                m = message(d, b, slot, False)
                m.wait_send()
                m.wait_recv()

                @functools.partial(each, CH)
                def _(c):
                    if d < 4:
                        for s in range(S):
                            v = recv_e[slot, d, c, s].astype(jnp.float32)[:T]
                            if dx == 0:
                                line(grid.at[q, s, c], -2 if dy < 0 else T + 1, 0, T, False)[...] = v
                            else:
                                line(grid.at[q, s, c], 0, -2 if dx < 0 else T + 1, T, True)[...] = v
                    else:
                        v = recv_k[slot, d - 4, c].astype(jnp.float32)
                        y0, x0 = (-2 if dy < 0 else T), (-2 if dx < 0 else T)
                        for s in range(S):
                            for k in range(2):
                                grid[q, s, c, pl.ds(at(y0 + k, x0), 2), :] = v[4 * s + 2 * k : 4 * s + 2 * k + 2]

    def init_messages(d, sending):
        e = opposite(d) if sending else d
        if d < 4:
            pairs = ((init_e.at[d], got_e.at[e], 0), (init_c.at[d], got_c.at[e], 1))
        else:
            pairs = ((init_k.at[d - 4], got_k.at[e - 4], 1),)
        return [
            pltpu.make_async_remote_copy(
                src_ref=src, dst_ref=dst,
                send_sem=isend_sem.at[k, d], recv_sem=irecv_sem.at[k, e],
                device_id=peer(d), device_id_type=MESH,
            )
            for src, dst, k in pairs
        ]

    @functools.partial(each, CH)
    def _(c):
        for s in range(S):
            for d in range(4):
                init_e[d, c, s] = edge_line(grid.at[0, s, c], d, 0)[...].astype(jnp.bfloat16)
                init_c[d, c, s] = edge_line(cgrid.at[s, c], d, 0)[...]
        for k in range(4):
            init_k[k, c] = jnp.zeros((8, LANES), jnp.float32)
            for s in range(S):
                start = at((k // 2) * (T - 1), (k % 2) * (T - 1))
                init_k[k, c, pl.ds(s, 1), :] = cgrid[s, c, pl.ds(start, 1), :]
        pack_messages(0, c, 0)

    pl.semaphore_wait(barrier, near)
    for d in range(8):

        @pl.when(exists(d))
        def _():
            for m in init_messages(d, True):
                m.start()
            message(d, 0, 0, True).start()

    for d in range(8):

        @pl.when(exists(d))
        def _():
            dy, dx = DIRS[d]
            for m in init_messages(d, False):
                m.wait_send()
                m.wait_recv()

            @functools.partial(each, CH)
            def _(c):
                for s in range(S):
                    y, x = (-1 if dy < 0 else T if dy > 0 else 0), (-1 if dx < 0 else T if dx > 0 else 0)
                    if d < 4:
                        line(grid.at[0, s, c], y, x, T, dy == 0)[...] = got_e[d, c, s].astype(jnp.float32)[:T]
                        line(cgrid.at[s, c], y, x, T, dy == 0)[...] = got_c[d, c, s][:T]
                    else:
                        cgrid[s, c, pl.ds(at(y, x), 1), :] = got_k[d - 4, c, pl.ds(s, 1), :]

    take_messages(0, 0, 0)

    @functools.partial(each, S * CH)
    def _(k):
        s, c = sample_chunk(k)
        for i in range(9):
            c_own[c, s, i] = gather_tile(cgrid.at[s, c], i // 3, i % 3)
        for k, (y, x, v) in enumerate(SIDES):
            c_ring[c, s, k] = line(cgrid.at[s, c], y, x, 16, v)[...]

    def build_tiles(q, inner):
        @functools.partial(each, S * CH)
        def _(k):
            s, c = sample_chunk(k)
            for ty in range(-1, 4):
                for tx in range(-1, 4):
                    if inner == (0 <= ty < 3 and 0 <= tx < 3):
                        v = gather_tile(grid.at[q, s, c], ty, tx)
                        pt[q, c, s, ty + 1, tx + 1] = v.astype(jnp.bfloat16)

    build_tiles(0, True)
    build_tiles(0, False)

    def ring_ok(k):
        r = lax.broadcasted_iota(jnp.int32, (16, LANES), 0)
        one = r >= 0
        if k == 2:
            return one & (my_col > 0)
        if k == 3:
            return one & (my_col < cols_n - 1)
        sides_ok = ((r > 0) | (my_col > 0)) & ((r < T + 1) | (my_col < cols_n - 1))
        return sides_ok & (one & ((my_row > 0) if k == 0 else (my_row < rows_n - 1)))

    def out_copy(b, t):
        return pltpu.make_async_copy(out_st.at[b], h_seq.at[t], out_sem.at[b])

    def own(t, cur):
        nxt = 1 - cur
        for c in range(CH):
            parts = [
                pt[cur, kc, :, tap // 3 : tap // 3 + 3, tap % 3 : tap % 3 + 3].reshape(S * 144, LANES)
                for tap in range(TAPS)
                for kc in range(CH)
            ]
            lhs = jnp.concatenate(parts, axis=1)
            gates = jnp.dot(lhs, w[c].reshape(TAPS * CDIM, 4 * LANES), preferred_element_type=jnp.float32)
            gates = gates + bias[c, pl.ds(t, 1), :]
            h, cn = lstm(gates, c_own[c].reshape(S * 144, LANES))
            c_own[c] = cn.reshape(S, 9, 16, LANES)
            pt[nxt, c, :, 1:4, 1:4] = h.reshape(S, 3, 3, 16, LANES)
            h_own[...] = h.astype(jnp.float32).reshape(S, 9, 16, LANES)

            @functools.partial(each, S)
            def _(s):
                for i in range(9):
                    scatter_tile(grid.at[nxt, s, c], i // 3, i % 3, h_own[s, i])

            @pl.when(t < STEPS - 2)
            def _():
                pack_messages(nxt, c, nxt)
                start_messages(c, nxt, lax.rem(t + 1, SLOTS))

        @pl.when(t >= 2)
        def _():
            out_copy(nxt, t).wait()

        @functools.partial(each, S * T)
        def _(k):
            s, y = lax.div(k, T), lax.rem(k, T)
            for c in range(CH):
                v = grid[nxt, s, c, pl.ds(at(y, 0), T), :]
                out_st[nxt, s, y, :, c * LANES : (c + 1) * LANES] = v.astype(jnp.bfloat16)

        out_copy(nxt, t).start()

    def ring(t, cur):
        nxt = 1 - cur

        @pl.when(t > 0)
        def _():
            take_messages(cur, cur, lax.rem(t, SLOTS))

        @functools.partial(each, S * CH)
        def _(j):
            s, c = sample_chunk(j)
            for k, (y, x, v) in enumerate(SIDES):
                for tap in range(TAPS):
                    a = line(grid.at[cur, s, c], y + tap // 3 - 1, x + tap % 3 - 1, 16, v)[...]
                    lhs_ring[tap, c, s, k] = a.astype(jnp.bfloat16)

        for c in range(CH):
            parts = [lhs_ring[tap, kc].reshape(S * 64, LANES) for tap in range(TAPS) for kc in range(CH)]
            gates = jnp.dot(
                jnp.concatenate(parts, axis=1),
                w[c].reshape(TAPS * CDIM, 4 * LANES),
                preferred_element_type=jnp.float32,
            )
            gates = gates + bias[c, pl.ds(t, 1), :]
            h, cn = lstm(gates, c_ring[c].reshape(S * 64, LANES))
            c_ring[c] = cn.reshape(S, 4, 16, LANES)
            h_ring[...] = h.astype(jnp.float32).reshape(S, 4, 16, LANES)

            @functools.partial(each, S)
            def _(s):
                for k, (y, x, v) in enumerate(SIDES):
                    m = jnp.where(ring_ok(k), h_ring[s, k], 0.0)
                    line(grid.at[nxt, s, c], y, x, SIDE_LEN[k], v)[...] = m[: SIDE_LEN[k]]

        build_tiles(nxt, False)

    for c in range(CH):
        pltpu.make_async_copy(w_hbm.at[:, :, :, pl.ds(0, 4 * LANES)], w.at[c], w_sem.at[c]).wait()

    @functools.partial(each, STEPS // 2)
    def _(k):
        own(2 * k, 0)
        ring(2 * k, 0)
        own(2 * k + 1, 1)

        @pl.when(k < STEPS // 2 - 1)
        def _():
            ring(2 * k + 1, 1)

    @functools.partial(each, S * CH)
    def _(k):
        s, c = sample_chunk(k)
        for i in range(9):
            scatter_tile(cgrid.at[s, c], i // 3, i % 3, c_own[c, s, i])

    @functools.partial(each, S * T)
    def _(k):
        s, y = lax.div(k, T), lax.rem(k, T)
        for c in range(CH):
            c_last[s, y, :, c * LANES : (c + 1) * LANES] = cgrid[s, c, pl.ds(at(y, 0), T), :]

    out_copy(1, STEPS - 2).wait()
    out_copy(0, STEPS - 1).wait()


def solution(mesh):
    def device_fn(h_init, c_init, w_rec, gate_bias):
        bias = gate_bias.reshape(STEPS, 4, CH, LANES).transpose(2, 0, 1, 3).reshape(CH, STEPS, 4 * LANES)
        vmem = pl.BlockSpec(memory_space=pltpu.VMEM)
        hbm = pl.BlockSpec(memory_space=pl.ANY)
        bf16, f32 = jnp.bfloat16, jnp.float32
        dma = pltpu.SemaphoreType.DMA
        return pl.pallas_call(
            kernel,
            out_shape=(
                jax.ShapeDtypeStruct((STEPS, S, T, T, CDIM), bf16),
                jax.ShapeDtypeStruct((S, T, T, CDIM), f32),
            ),
            in_specs=[vmem, vmem, hbm, vmem],
            out_specs=(hbm, vmem),
            scratch_shapes=[
                pltpu.VMEM((CH, 3, 3, CDIM, 4 * LANES), bf16),
                pltpu.VMEM((2, CH, S, 5, 5, 16, LANES), bf16),
                pltpu.VMEM((2, S, CH, GROWS, LANES), f32),
                pltpu.VMEM((S, CH, GROWS, LANES), f32),
                pltpu.VMEM((CH, S, 9, 16, LANES), f32),
                pltpu.VMEM((CH, S, 4, 16, LANES), f32),
                pltpu.VMEM((TAPS, CH, S, 4, 16, LANES), bf16),
                pltpu.VMEM((2, S, T, T, CDIM), bf16),
                pltpu.VMEM((S, 9, 16, LANES), f32),
                pltpu.VMEM((S, 4, 16, LANES), f32),
                pltpu.VMEM((2, 4, CH, S, 16, LANES), bf16),
                pltpu.VMEM((2, 4, CH, 8, LANES), bf16),
                pltpu.VMEM((SLOTS, 4, CH, S, 16, LANES), bf16),
                pltpu.VMEM((SLOTS, 4, CH, 8, LANES), bf16),
                pltpu.VMEM((4, CH, S, 16, LANES), bf16),
                pltpu.VMEM((4, CH, S, 16, LANES), f32),
                pltpu.VMEM((4, CH, 8, LANES), f32),
                pltpu.VMEM((4, CH, S, 16, LANES), bf16),
                pltpu.VMEM((4, CH, S, 16, LANES), f32),
                pltpu.VMEM((4, CH, 8, LANES), f32),
                pltpu.VMEM((4, 8, LANES), f32),
                dma((CH,)),
                dma((2,)),
                dma((2, 8)),
                dma((SLOTS, 8)),
                dma((2, 8)),
                dma((2, 8)),
            ],
            compiler_params=pltpu.CompilerParams(
                collective_id=0, has_side_effects=True, vmem_limit_bytes=60 * 1024 * 1024
            ),
        )(h_init, c_init, w_rec, bias)

    state_spec = P("dp", "rows", "cols", None)
    return jax.shard_map(
        device_fn,
        mesh=mesh,
        in_specs=(state_spec, state_spec, P(), P()),
        out_specs=(P(None, "dp", "rows", "cols", None), state_spec),
        check_vma=False,
    )
```

```python
import jax
import jax.numpy as jnp
from jax import lax
from jax.experimental import pallas as pl
from jax.experimental.pallas import tpu as pltpu
from jax.sharding import PartitionSpec as P

MESH = pl.DeviceIdType.MESH
STEPS = 12
S = 2
T = 12
LANES = 128
CH = 3
CDIM = CH * LANES
TAPS = 9
KDIM = TAPS * CDIM
SLOTS = 4

YPITCH = 3 * 6 * S
GROWS = 20 * YPITCH
RTILES = 7

DIRS = ((-1, 0), (1, 0), (0, -1), (0, 1), (-1, -1), (-1, 1), (1, -1), (1, 1))


def opposite(d):
    dy, dx = DIRS[d]
    return DIRS.index((-dy, -dx))


def at(y, x):
    return ((y + 2) * 3 + (x + 2) % 3) * 6 * S + (x + 2) // 3 * S


def sigmoid(v):
    return 0.5 * jnp.tanh(0.5 * v) + 0.5


def lstm(gates, bias, c_prev):
    i, f, o, g = (gates[:, k * LANES : (k + 1) * LANES] + bias[k] for k in range(4))
    c = sigmoid(f) * c_prev + sigmoid(i) * jnp.tanh(g)
    h = (sigmoid(o) * jnp.tanh(c)).astype(jnp.bfloat16)
    return h, c


def side_rows(dy):
    return -1 if dy < 0 else T


def ring_rows(g, dy, dx):
    sub = lax.broadcasted_iota(jnp.int32, (8, LANES), 0)
    out = []
    for ix in range(3):
        for y in (-1, T):
            out.append(g[pl.ds(at(y + dy, ix + dx), 8), :])
    for x in (-1, T):
        for s in range(S):
            out.append(g[pl.ds(at(dy, x + dx) + s, 8, stride=YPITCH), :])
    for x in (-1, T):
        a = g[pl.ds(at(8 + dy, x + dx), 8, stride=YPITCH), :]
        b = g[pl.ds(at(4 + dy, x + dx) + 1, 8, stride=YPITCH), :]
        out.append(jnp.where(sub < 4, a, b))
    v = None
    for k, (y, x) in enumerate(((-1, -1), (-1, T), (T, -1), (T, T))):
        a = g[pl.ds(at(y + dy, x + dx) - 2 * k, 8), :]
        v = a if v is None else jnp.where(sub < 2 * k, v, a)
    return out + [v, v]


def put_ring(g, v):
    k = 0
    for ix in range(3):
        for y in (-1, T):
            g[pl.ds(at(y, ix), 8), :] = v[k]
            k += 1
    for x in (-1, T):
        for s in range(S):
            g[pl.ds(at(0, x) + s, 8, stride=YPITCH), :] = v[k]
            k += 1
    for x in (-1, T):
        for s in range(S):
            g[pl.ds(at(8, x) + s, 4, stride=YPITCH), :] = v[k][4 * s : 4 * s + 4]
        k += 1
    for j, (y, x) in enumerate(((-1, -1), (-1, T), (T, -1), (T, T))):
        g[pl.ds(at(y, x), 2), :] = v[k][2 * j : 2 * j + 2]


def put_line(g, d, dist, v):
    dy, dx = DIRS[d]
    if dx == 0:
        y = -dist if dy < 0 else T - 1 + dist
        for ix in range(3):
            g[pl.ds(at(y, ix), 8), :] = v[8 * ix : 8 * ix + 8]
    else:
        x = -dist if dx < 0 else T - 1 + dist
        for k in range(T):
            g[pl.ds(at(6 * (k % 2) + k // 2, x), 2), :] = v[2 * k : 2 * k + 2]


def kernel(
    h_init, c_init, w_hbm, bias_hbm, h_seq, c_last,
    w, bias, pt, grid, cgrid, h_new, c_own, c_ring, lhs_ring,
    recv_v, recv_h, recv_k, first_v, first_h, first_k, firstc_v, firstc_h, firstc_k,
    w_sem, in_sem, out_sem, send_sem, recv_sem, fsend_sem, frecv_sem,
):
    rows_n, cols_n = lax.axis_size("rows"), lax.axis_size("cols")
    my_row, my_col = lax.axis_index("rows"), lax.axis_index("cols")
    f32, bf16 = jnp.float32, jnp.bfloat16

    pt_rows = pt.reshape(CH, 8, 5, 16, LANES)
    own_rows = c_own.reshape(CH, S * T * T, LANES)
    lines = {0: recv_v.reshape(SLOTS, 2, CH, 32, LANES), 1: recv_h.reshape(SLOTS, 2, CH, 32, LANES)}
    corners = recv_k.reshape(SLOTS, 4, CH, 16, LANES)

    def lacks(d):
        dy, dx = DIRS[d]
        r = jnp.bool_(False) if dy == 0 else my_row == (0 if dy < 0 else rows_n - 1)
        c = jnp.bool_(False) if dx == 0 else my_col == (0 if dx < 0 else cols_n - 1)
        return r, c, jnp.logical_or(r, c)

    def flip(v):
        return v + 1 - 2 * lax.rem(v, 2)

    def peer(d, back):
        dy, dx = DIRS[d]
        lr, lc, lack = lacks(d)
        if dx == 0:
            r, c = my_row, flip(my_col)
        elif dy == 0:
            r, c = flip(my_row), my_col
        else:
            a = my_row if dy < 0 else rows_n - 1 - my_row
            b = my_col if dx < 0 else cols_n - 1 - my_col
            on_c = jnp.logical_and(lc, a >= 2)
            on_r = jnp.logical_and(lr, b >= 2)
            if back:
                a3, b3 = jnp.where(a == 1, 0, jnp.where(b == 1, 0, 1)), jnp.where(a == 1, 1, 0)
            else:
                a3, b3 = jnp.where(b == 1, 1, 0), jnp.where(jnp.logical_and(a == 0, b == 0), 1, 0)
            a2 = jnp.where(on_c, flip(a), jnp.where(on_r, 0, a3))
            b2 = jnp.where(on_c, 0, jnp.where(on_r, flip(b), b3))
            r = a2 if dy < 0 else rows_n - 1 - a2
            c = b2 if dx < 0 else cols_n - 1 - b2
        return {"rows": jnp.where(lack, r, my_row + dy), "cols": jnp.where(lack, c, my_col + dx)}

    lack = [lacks(d)[2] for d in range(8)]
    peers = [peer(d, False) for d in range(8)]
    landing = [jnp.where(lack[d], d, opposite(d)) for d in range(8)]

    def kept(d, v):
        return jnp.where(lack[d], jnp.zeros_like(v), v)

    def edge_cells(d, depth):
        dy, dx = DIRS[d]
        if dx == 0:
            return (depth, slice(0, 3), 0, slice(0, 4)) if dy < 0 else (5 - depth, slice(0, 3), 1, slice(0, 4))
        return (slice(0, 6), depth, slice(0, 2), 0) if dx < 0 else (slice(0, 6), 2 - depth, slice(0, 2), 3)

    def corner_cells(d, n):
        dy, dx = DIRS[d]
        iy, jy = (slice(0, n), 0) if dy < 0 else (slice(6 - n, 6), 1)
        ix, jx = (slice(0, n), 0) if dx < 0 else (slice(3 - n, 3), 3)
        return iy, ix, jy, jx

    def moved(i, k):
        return slice(i.start + k, i.stop + k) if isinstance(i, slice) else i + k

    def tile_cells(cells):
        iy, ix, jy, jx = cells
        return pt.at[:, moved(iy, 1), moved(ix, 1), jy, jx]

    def remote(d, src, dst, dst_back, ssem, rsem, rsem_back, sending):
        return pltpu.make_async_remote_copy(
            src_ref=src, dst_ref=dst if sending else dst_back,
            send_sem=ssem, recv_sem=rsem if sending else rsem_back,
            device_id=peers[d], device_id_type=MESH,
        )

    def message(d, slot, sending):
        e = landing[d]
        if d < 2:
            src, dst = tile_cells(edge_cells(d, 1)), lambda k: recv_v.at[slot, k, :, 0:3]
        elif d < 4:
            src, dst = tile_cells(edge_cells(d, 1)), lambda k: recv_h.at[slot, k - 2, :, 0:6]
        else:
            src, dst = tile_cells(corner_cells(d, 2)), lambda k: recv_k.at[slot, k - 4, :, 0:2]
        return remote(
            d, src, dst(e), dst(d), send_sem.at[d], recv_sem.at[slot, e], recv_sem.at[slot, d], sending
        )

    def first_message(d, k, sending):
        e = landing[d]
        cells = edge_cells(d, 0) if d < 4 else corner_cells(d, 1)
        src = tile_cells(cells) if k == 0 else c_own.at[(slice(None),) + cells]
        if d < 2:
            dst = lambda j: (firstc_v if k else first_v).at[j, :, 0:3]
        elif d < 4:
            dst = lambda j: (firstc_h if k else first_h).at[j - 2, :, 0:6]
        else:
            dst = lambda j: (firstc_k if k else first_k).at[j - 4, :, 0:1, 0:1]
        return remote(
            d, src, dst(e), dst(d), fsend_sem.at[k, d], frecv_sem.at[k, e], frecv_sem.at[k, d], sending
        )

    def tile_copy(hbm, vmem, sem, out):
        for c in range(CH):
            for ix in range(3):
                for jy in range(2):
                    a, b = hbm.at[jy, :, :, ix, :, pl.ds(c * LANES, LANES)], vmem(c, ix, jy)
                    pltpu.make_async_copy(b if out else a, a if out else b, sem).start()

    def tile_wait(hbm, vmem, sem, out):
        for c in range(CH):
            for ix in range(3):
                for jy in range(2):
                    a, b = hbm.at[jy, :, :, ix, :, pl.ds(c * LANES, LANES)], vmem(c, ix, jy)
                    pltpu.make_async_copy(b if out else a, a if out else b, sem).wait()

    def h_tiles(c, ix, jy):
        return pt.at[c, 1:7, 1 + ix, jy]

    def c_tiles(c, ix, jy):
        return c_own.at[c, :, ix, jy]

    tile_copy(h_init, h_tiles, in_sem.at[0], False)
    tile_copy(c_init, c_tiles, in_sem.at[1], False)
    bias_copies = [
        pltpu.make_async_copy(bias_hbm.at[:, pl.ds(k * LANES, LANES)], bias.at[k], in_sem.at[2]) for k in range(4 * CH)
    ]
    for m in bias_copies:
        m.start()
    for c in range(CH):
        for kc in range(CH):
            for g in range(4):
                pltpu.make_async_copy(
                    w_hbm.at[:, :, pl.ds(kc * LANES, LANES), pl.ds(g * CDIM + c * LANES, LANES)],
                    w.at[c, kc, :, :, :, pl.ds(g * LANES, LANES)],
                    w_sem.at[c],
                ).start()

    def w_wait(c):
        pltpu.make_async_copy(w.at[c], w.at[c], w_sem.at[c]).wait()

    barrier = pltpu.get_barrier_semaphore()
    for d in range(8):
        pl.semaphore_signal(barrier, inc=1, device_id=peer(d, True), device_id_type=MESH)

    tile_wait(h_init, h_tiles, in_sem.at[0], False)
    pl.semaphore_wait(barrier, 8)
    for d in range(8):
        first_message(d, 0, True).start()
    for d in range(8):
        message(d, 0, True).start()
    tile_wait(c_init, c_tiles, in_sem.at[1], False)
    for d in range(8):
        first_message(d, 1, True).start()
    tile_copy(h_seq.at[STEPS - 1], h_tiles, out_sem, True)

    def put_own(g, hf):
        k = 0
        for iy in range(6):
            for ix in range(3):
                for jy in range(2):
                    g[pl.ds(at(6 * jy + iy, ix), 8), :] = hf[k : k + 8]
                    k += 8

    for c in range(CH):
        put_own(grid.at[c], pt_rows[c, 1:7, 1:4].reshape(S * T * T, LANES).astype(f32))

    def take_first(k, to, gv, gh, gk):
        for d in range(8):
            first_message(d, k, False).wait_recv()
        gv, gh, gk = gv.reshape(2, CH, 32, LANES), gh.reshape(2, CH, 32, LANES), gk.reshape(4, CH, 16, LANES)
        for c in range(CH):
            g = to.at[c]
            for d in range(4):
                v = (gv if d < 2 else gh)[d % 2, c].astype(f32)
                put_line(g, d, 1, kept(d, v[: 2 * T]))
            for d in range(4, 8):
                v = kept(d, gk[d - 4, c].astype(f32)[:8])
                dy, dx = DIRS[d]
                g[pl.ds(at(side_rows(dy), side_rows(dx)), 2), :] = v[:2]

    def build_border(c):
        g = grid.at[c]
        for ty in range(-1, 7):
            for tx in range(-1, 4):
                if not (0 <= ty < 6 and 0 <= tx < 3):
                    v = jnp.concatenate([g[pl.ds(at(ty + 6 * jy, tx), 8), :] for jy in range(2)], axis=0)
                    pt_rows[c, ty + 1, tx + 1] = v.astype(bf16)

    take_first(0, grid, first_v, first_h, first_k)
    for d in range(8):
        first_message(d, 0, False).wait_send()
        first_message(d, 1, False).wait_send()
    for c in range(CH):
        build_border(c)
    for m in bias_copies:
        m.wait()

    def bias_of(t, c):
        return [bias[g * CH + c, pl.ds(t, 1), :] for g in range(4)]

    def own(t, c):
        parts = [
            pt_rows[kc, tap // 3 : tap // 3 + 6, tap % 3 : tap % 3 + 3].reshape(S * T * T, LANES)
            for kc in range(CH)
            for tap in range(TAPS)
        ]
        gates = jnp.dot(
            jnp.concatenate(parts, axis=1), w[c].reshape(KDIM, 4 * LANES), preferred_element_type=f32
        )
        h, cn = lstm(gates, bias_of(t, c), own_rows[c])
        own_rows[c] = cn
        h_new[c] = h

    def take(slot):
        for d in range(8):
            message(d, slot, False).wait_recv()
        for c in range(CH):
            g = grid.at[c]
            for d in range(4):
                put_line(g, d, 2, kept(d, lines[d // 2][slot, d % 2, c].astype(f32)[: 2 * T]))
            for d in range(4, 8):
                v = kept(d, corners[slot, d - 4, c].astype(f32)[:8])
                dy, dx = DIRS[d]
                y0, x0 = (-2 if dy < 0 else T), (-2 if dx < 0 else T)
                for k in range(4):
                    y, x = y0 + k // 2, x0 + k % 2
                    if (y, x) != (side_rows(dy), side_rows(dx)):
                        g[pl.ds(at(y, x), 2), :] = v[2 * k : 2 * k + 2]

    def ring_mask():
        sub = lax.broadcasted_iota(jnp.int32, (8, LANES), 0)
        ok = [jnp.where(lack[d], 0.0, 1.0).astype(f32) for d in range(8)]
        full = lambda v: jnp.full((8, LANES), v, f32)
        out = [full(ok[0]), full(ok[1])] * 3 + [full(ok[2])] * 2 + [full(ok[3])] * 2 + [full(ok[2]), full(ok[3])]
        k = full(ok[7])
        for j in (2, 1, 0):
            k = jnp.where(sub < 2 * (j + 1), full(ok[4 + j]), k)
        return out + [k]

    def ring(t):
        mask = ring_mask()
        for c in range(CH):
            parts = [lhs_ring[kc, tap] for kc in range(CH) for tap in range(TAPS)]
            gates = jnp.dot(
                jnp.concatenate(parts, axis=1), w[c].reshape(KDIM, 4 * LANES), preferred_element_type=f32
            )
            h, cn = lstm(gates, bias_of(t, c), c_ring[c])
            c_ring[c] = cn
            hf = h.astype(f32)
            put_ring(grid.at[c], [hf[8 * k : 8 * k + 8] * m for k, m in enumerate(mask)])
            build_border(c)

    def put_new(t):
        tile_wait(h_seq.at[STEPS - 1], h_tiles, out_sem, True)
        for c in range(CH):
            pt_rows[c, 1:7, 1:4] = h_new[c].reshape(6, 3, 16, LANES)
        tile_copy(h_seq.at[t], h_tiles, out_sem, True)

    def step(t, carry):
        own(t, 1)
        own(t, 2)
        for d in range(8):
            message(d, lax.rem(t, SLOTS), True).wait_send()
        put_new(t)
        for d in range(8):
            message(d, lax.rem(t + 1, SLOTS), True).start()
        take(lax.rem(t, SLOTS))
        for kc in range(CH):
            for tap in range(TAPS):
                v = ring_rows(grid.at[kc], tap // 3 - 1, tap % 3 - 1)
                lhs_ring[kc, tap] = jnp.concatenate(v, axis=0).astype(bf16)
        for c in range(CH):
            put_own(grid.at[c], h_new[c].astype(f32))
        ring(t)
        own(t + 1, 0)
        return carry

    w_wait(0)
    own(0, 0)
    take_first(1, cgrid, firstc_v, firstc_h, firstc_k)
    for c in range(CH):
        c_ring[c] = jnp.concatenate(ring_rows(cgrid.at[c], 0, 0), axis=0)
    w_wait(1)
    w_wait(2)

    lax.fori_loop(0, STEPS - 1, step, 0)
    own(STEPS - 1, 1)
    own(STEPS - 1, 2)
    tile_copy(c_last, c_tiles, in_sem.at[1], True)
    for d in range(8):
        m = message(d, (STEPS - 1) % SLOTS, False)
        m.wait_send()
        m.wait_recv()
    put_new(STEPS - 1)
    tile_wait(h_seq.at[STEPS - 1], h_tiles, out_sem, True)
    tile_wait(c_last, c_tiles, in_sem.at[1], True)


def solution(mesh):
    def device_fn(h_init, c_init, w_rec, gate_bias):
        hbm = pl.BlockSpec(memory_space=pl.ANY)
        bf16, f32 = jnp.bfloat16, jnp.float32
        dma = pltpu.SemaphoreType.DMA
        tiles = (2, 6, 4, 3, S, CDIM)
        h_seq, c_last = pl.pallas_call(
            kernel,
            out_shape=(jax.ShapeDtypeStruct((STEPS,) + tiles, bf16), jax.ShapeDtypeStruct(tiles, f32)),
            in_specs=[hbm] * 4,
            out_specs=(hbm, hbm),
            scratch_shapes=[
                pltpu.VMEM((CH, CH, 3, 3, LANES, 4 * LANES), bf16),
                pltpu.VMEM((4 * CH, STEPS, LANES), f32),
                pltpu.VMEM((CH, 8, 5, 2, 4, S, LANES), bf16),
                pltpu.VMEM((CH, GROWS, LANES), f32),
                pltpu.VMEM((CH, GROWS, LANES), f32),
                pltpu.VMEM((CH, S * T * T, LANES), bf16),
                pltpu.VMEM((CH, 6, 3, 2, 4, S, LANES), f32),
                pltpu.VMEM((CH, RTILES * 16, LANES), f32),
                pltpu.VMEM((CH, TAPS, RTILES * 16, LANES), bf16),
                pltpu.VMEM((SLOTS, 2, CH, 4, 4, S, LANES), bf16),
                pltpu.VMEM((SLOTS, 2, CH, 8, 2, S, LANES), bf16),
                pltpu.VMEM((SLOTS, 4, CH, 4, 2, S, LANES), bf16),
                pltpu.VMEM((2, CH, 4, 4, S, LANES), bf16),
                pltpu.VMEM((2, CH, 8, 2, S, LANES), bf16),
                pltpu.VMEM((4, CH, 4, 2, S, LANES), bf16),
                pltpu.VMEM((2, CH, 4, 4, S, LANES), f32),
                pltpu.VMEM((2, CH, 8, 2, S, LANES), f32),
                pltpu.VMEM((4, CH, 4, 2, S, LANES), f32),
                dma((CH,)),
                dma((3,)),
                dma,
                dma((8,)),
                dma((SLOTS, 8)),
                dma((2, 8)),
                dma((2, 8)),
            ],
            compiler_params=pltpu.CompilerParams(
                collective_id=0, has_side_effects=True, vmem_limit_bytes=60 * 1024 * 1024
            ),
        )(
            h_init.transpose(1, 2, 0, 3).reshape(tiles),
            c_init.transpose(1, 2, 0, 3).reshape(tiles),
            w_rec,
            gate_bias,
        )
        h_seq = h_seq.reshape(STEPS, T, T, S, CDIM).transpose(0, 3, 1, 2, 4)
        return h_seq, c_last.reshape(T, T, S, CDIM).transpose(2, 0, 1, 3)

    state_spec = P("dp", "rows", "cols", None)
    return jax.shard_map(
        device_fn,
        mesh=mesh,
        in_specs=(state_spec, state_spec, P(), P()),
        out_specs=(P(None, "dp", "rows", "cols", None), state_spec),
        check_vma=False,
    )
```

```python
import jax
import jax.numpy as jnp
from jax import lax
from jax.experimental import pallas as pl
from jax.experimental.pallas import tpu as pltpu
from jax.sharding import PartitionSpec as P

MESH = pl.DeviceIdType.MESH
STEPS = 12
S = 2
T = 12
LANES = 128
CH = 3
CDIM = CH * LANES
TAPS = 9
KDIM = TAPS * CDIM
SLOTS = 4

YPITCH = 3 * 6 * S
GROWS = 20 * YPITCH
RTILES = 7

DIRS = ((-1, 0), (1, 0), (0, -1), (0, 1), (-1, -1), (-1, 1), (1, -1), (1, 1))


def opposite(d):
    dy, dx = DIRS[d]
    return DIRS.index((-dy, -dx))


def at(y, x):
    return ((y + 2) * 3 + (x + 2) % 3) * 6 * S + (x + 2) // 3 * S


def sigmoid(v):
    return 0.5 * jnp.tanh(0.5 * v) + 0.5


def lstm(gates, bias, c_prev):
    i, f, o, g = (gates[:, k * LANES : (k + 1) * LANES] + bias[k] for k in range(4))
    c = sigmoid(f) * c_prev + sigmoid(i) * jnp.tanh(g)
    h = (sigmoid(o) * jnp.tanh(c)).astype(jnp.bfloat16)
    return h, c


def side_rows(dy):
    return -1 if dy < 0 else T


def ring_rows(g, dy, dx):
    sub = lax.broadcasted_iota(jnp.int32, (8, LANES), 0)
    out = []
    for ix in range(3):
        for y in (-1, T):
            out.append(g[pl.ds(at(y + dy, ix + dx), 8), :])
    for x in (-1, T):
        for s in range(S):
            out.append(g[pl.ds(at(dy, x + dx) + s, 8, stride=YPITCH), :])
    for x in (-1, T):
        a = g[pl.ds(at(8 + dy, x + dx), 8, stride=YPITCH), :]
        b = g[pl.ds(at(4 + dy, x + dx) + 1, 8, stride=YPITCH), :]
        out.append(jnp.where(sub < 4, a, b))
    v = None
    for k, (y, x) in enumerate(((-1, -1), (-1, T), (T, -1), (T, T))):
        a = g[pl.ds(at(y + dy, x + dx) - 2 * k, 8), :]
        v = a if v is None else jnp.where(sub < 2 * k, v, a)
    return out + [v, v]


def put_ring(g, v):
    k = 0
    for ix in range(3):
        for y in (-1, T):
            g[pl.ds(at(y, ix), 8), :] = v[k]
            k += 1
    for x in (-1, T):
        for s in range(S):
            g[pl.ds(at(0, x) + s, 8, stride=YPITCH), :] = v[k]
            k += 1
    for x in (-1, T):
        for s in range(S):
            g[pl.ds(at(8, x) + s, 4, stride=YPITCH), :] = v[k][4 * s : 4 * s + 4]
        k += 1
    for j, (y, x) in enumerate(((-1, -1), (-1, T), (T, -1), (T, T))):
        g[pl.ds(at(y, x), 2), :] = v[k][2 * j : 2 * j + 2]


def lanes(c):
    return slice(c * LANES, (c + 1) * LANES)


def line_pieces(line, c):
    if line.shape[0] == 4:
        return [line[:, ix, :, lanes(c)].reshape(8, LANES) for ix in range(3)]
    return [line[jy, :, :, lanes(c)].reshape(12, LANES) for jy in range(2)]


def put_line(g, d, dist, pieces):
    dy, dx = DIRS[d]
    if dx == 0:
        y = -dist if dy < 0 else T - 1 + dist
        for ix in range(3):
            g[pl.ds(at(y, ix), 8), :] = pieces[ix]
    else:
        x = -dist if dx < 0 else T - 1 + dist
        for jy in range(2):
            for iy in range(6):
                g[pl.ds(at(6 * jy + iy, x), 2), :] = pieces[jy][2 * iy : 2 * iy + 2]


def put_cells(ref, c, v):
    k = 0
    for iy in range(6):
        for ix in range(3):
            for jy in range(2):
                ref[jy, iy, :, ix, :, lanes(c)] = v[k : k + 8].reshape(4, S, LANES)
                k += 8


def get_cells(ref, c):
    return jnp.concatenate(
        [
            ref[jy, iy, :, ix, :, lanes(c)].reshape(8, LANES)
            for iy in range(6)
            for ix in range(3)
            for jy in range(2)
        ],
        axis=0,
    )


def kernel(
    h_init, c_init, w_hbm, bias_hbm, h_seq, c_last,
    w, bias, pt, grid, cgrid, h_new, h_dma, c_own, c_dma, c_ring, lhs_ring,
    recv_v, recv_h, recv_k, first_v, first_h, first_k, firstc_v, firstc_h, firstc_k,
    w_sem, in_sem, out_sem, send_sem, recv_sem, fsend_sem, frecv_sem,
):
    rows_n, cols_n = lax.axis_size("rows"), lax.axis_size("cols")
    my_row, my_col = lax.axis_index("rows"), lax.axis_index("cols")
    f32, bf16 = jnp.float32, jnp.bfloat16

    def lacks(d):
        dy, dx = DIRS[d]
        r = jnp.bool_(False) if dy == 0 else my_row == (0 if dy < 0 else rows_n - 1)
        c = jnp.bool_(False) if dx == 0 else my_col == (0 if dx < 0 else cols_n - 1)
        return r, c, jnp.logical_or(r, c)

    def flip(v):
        return v + 1 - 2 * lax.rem(v, 2)

    def peer(d, back):
        dy, dx = DIRS[d]
        lr, lc, lack = lacks(d)
        if dx == 0:
            r, c = my_row, flip(my_col)
        elif dy == 0:
            r, c = flip(my_row), my_col
        else:
            a = my_row if dy < 0 else rows_n - 1 - my_row
            b = my_col if dx < 0 else cols_n - 1 - my_col
            on_c = jnp.logical_and(lc, a >= 2)
            on_r = jnp.logical_and(lr, b >= 2)
            if back:
                a3, b3 = jnp.where(a == 1, 0, jnp.where(b == 1, 0, 1)), jnp.where(a == 1, 1, 0)
            else:
                a3, b3 = jnp.where(b == 1, 1, 0), jnp.where(jnp.logical_and(a == 0, b == 0), 1, 0)
            a2 = jnp.where(on_c, flip(a), jnp.where(on_r, 0, a3))
            b2 = jnp.where(on_c, 0, jnp.where(on_r, flip(b), b3))
            r = a2 if dy < 0 else rows_n - 1 - a2
            c = b2 if dx < 0 else cols_n - 1 - b2
        return {"rows": jnp.where(lack, r, my_row + dy), "cols": jnp.where(lack, c, my_col + dx)}

    lack = [lacks(d)[2] for d in range(8)]
    peers = [peer(d, False) for d in range(8)]
    landing = [jnp.where(lack[d], d, opposite(d)) for d in range(8)]

    def kept(d, v):
        return jnp.where(lack[d], jnp.zeros_like(v), v)

    def edge_cells(d, depth):
        dy, dx = DIRS[d]
        every = slice(None)
        if dx == 0:
            return (0, depth, every, every) if dy < 0 else (1, 5 - depth, every, every)
        return (every, every, 0, depth) if dx < 0 else (every, every, 3, 2 - depth)

    def corner_cells(d, n):
        dy, dx = DIRS[d]
        jy, iy = (0, slice(0, n)) if dy < 0 else (1, slice(6 - n, 6))
        jx, ix = (0, slice(0, n)) if dx < 0 else (3, slice(3 - n, 3))
        return jy, iy, jx, ix

    def remote(d, src, dst, dst_back, ssem, rsem, rsem_back, sending):
        return pltpu.make_async_remote_copy(
            src_ref=src, dst_ref=dst if sending else dst_back,
            send_sem=ssem, recv_sem=rsem if sending else rsem_back,
            device_id=peers[d], device_id_type=MESH,
        )

    def message(d, slot, sending):
        e = landing[d]
        if d < 2:
            src, dst = h_dma.at[edge_cells(d, 1)], lambda k: recv_v.at[slot, k]
        elif d < 4:
            src, dst = h_dma.at[edge_cells(d, 1)], lambda k: recv_h.at[slot, k - 2]
        else:
            src, dst = h_dma.at[corner_cells(d, 2)], lambda k: recv_k.at[slot, k - 4]
        return remote(
            d, src, dst(e), dst(d), send_sem.at[d], recv_sem.at[slot, e], recv_sem.at[slot, d], sending
        )

    def first_message(d, k, sending):
        e = landing[d]
        cells = edge_cells(d, 0) if d < 4 else corner_cells(d, 1)
        src = (c_dma if k else h_dma).at[cells]
        if d < 2:
            dst = lambda j: (firstc_v if k else first_v).at[j]
        elif d < 4:
            dst = lambda j: (firstc_h if k else first_h).at[j - 2]
        else:
            dst = lambda j: (firstc_k if k else first_k).at[j - 4]
        return remote(
            d, src, dst(e), dst(d), fsend_sem.at[k, d], frecv_sem.at[k, e], frecv_sem.at[k, d], sending
        )

    h_in = pltpu.make_async_copy(h_init, h_dma, in_sem.at[0])
    c_in = pltpu.make_async_copy(c_init, c_dma, in_sem.at[1])
    c_out = pltpu.make_async_copy(c_dma, c_last, in_sem.at[1])

    def h_out(t):
        return pltpu.make_async_copy(h_dma, h_seq.at[t], out_sem)

    h_in.start()
    c_in.start()
    bias_copies = [
        pltpu.make_async_copy(bias_hbm.at[:, pl.ds(k * LANES, LANES)], bias.at[k], in_sem.at[2]) for k in range(4 * CH)
    ]
    for m in bias_copies:
        m.start()
    for c in range(CH):
        for kc in range(CH):
            for g in range(4):
                pltpu.make_async_copy(
                    w_hbm.at[:, :, pl.ds(kc * LANES, LANES), pl.ds(g * CDIM + c * LANES, LANES)],
                    w.at[c, kc, :, :, :, pl.ds(g * LANES, LANES)],
                    w_sem.at[c],
                ).start()

    def w_wait(c):
        pltpu.make_async_copy(w.at[c], w.at[c], w_sem.at[c]).wait()

    barrier = pltpu.get_barrier_semaphore()
    for d in range(8):
        pl.semaphore_signal(barrier, inc=1, device_id=peer(d, True), device_id_type=MESH)

    h_in.wait()
    pl.semaphore_wait(barrier, 8)
    for d in range(8):
        first_message(d, 0, True).start()
    for d in range(8):
        message(d, 0, True).start()
    c_in.wait()
    for d in range(8):
        first_message(d, 1, True).start()
    for c in range(CH):
        c_own[c] = get_cells(c_dma, c)
    h_out(STEPS - 1).start()

    def put_own(g, hf):
        k = 0
        for iy in range(6):
            for ix in range(3):
                for jy in range(2):
                    g[pl.ds(at(6 * jy + iy, ix), 8), :] = hf[k : k + 8]
                    k += 8

    for c in range(CH):
        h = get_cells(h_dma, c)
        pt[c, 1:7, 1:4] = h.reshape(6, 3, 16, LANES)
        put_own(grid.at[c], h.astype(f32))

    def take_first(k, to, gv, gh, gk):
        for d in range(8):
            first_message(d, k, False).wait_recv()
        for c in range(CH):
            g = to.at[c]
            for d in range(4):
                v = line_pieces((gv if d < 2 else gh).at[d % 2], c)
                put_line(g, d, 1, [kept(d, a.astype(f32)) for a in v])
            for d in range(4, 8):
                v = gk[d - 4, 0, 0, :, lanes(c)].astype(f32)
                dy, dx = DIRS[d]
                g[pl.ds(at(side_rows(dy), side_rows(dx)), 2), :] = kept(d, v)

    def build_border(c):
        g = grid.at[c]
        for ty in range(-1, 7):
            for tx in range(-1, 4):
                if not (0 <= ty < 6 and 0 <= tx < 3):
                    v = jnp.concatenate([g[pl.ds(at(ty + 6 * jy, tx), 8), :] for jy in range(2)], axis=0)
                    pt[c, ty + 1, tx + 1] = v.astype(bf16)

    take_first(0, grid, first_v, first_h, first_k)
    for d in range(8):
        first_message(d, 0, False).wait_send()
    for c in range(CH):
        build_border(c)
    for m in bias_copies:
        m.wait()

    def bias_of(t, c):
        return [bias[g * CH + c, pl.ds(t, 1), :] for g in range(4)]

    def own(t, c, lo=0, hi=6):
        n = (hi - lo) * 48
        parts = [
            pt[kc, lo + tap // 3 : hi + tap // 3, tap % 3 : tap % 3 + 3].reshape(n, LANES)
            for kc in range(CH)
            for tap in range(TAPS)
        ]
        gates = jnp.dot(
            jnp.concatenate(parts, axis=1), w[c].reshape(KDIM, 4 * LANES), preferred_element_type=f32
        )
        rows = pl.ds(lo * 48, n)
        h, cn = lstm(gates, bias_of(t, c), c_own[c, rows])
        c_own[c, rows] = cn
        h_new[c, rows] = h

    def take(slot):
        for d in range(8):
            message(d, slot, False).wait_recv()
        for c in range(CH):
            g = grid.at[c]
            for d in range(4):
                v = line_pieces((recv_v if d < 2 else recv_h).at[slot, d % 2], c)
                put_line(g, d, 2, [kept(d, a.astype(f32)) for a in v])
            for d in range(4, 8):
                v = kept(d, recv_k[slot, d - 4, :, :, :, lanes(c)].reshape(8, LANES).astype(f32))
                dy, dx = DIRS[d]
                y0, x0 = (-2 if dy < 0 else T), (-2 if dx < 0 else T)
                for k in range(4):
                    y, x = y0 + k // 2, x0 + k % 2
                    if (y, x) != (side_rows(dy), side_rows(dx)):
                        g[pl.ds(at(y, x), 2), :] = v[2 * k : 2 * k + 2]

    def ring_mask():
        sub = lax.broadcasted_iota(jnp.int32, (8, LANES), 0)
        ok = [jnp.where(lack[d], 0.0, 1.0).astype(f32) for d in range(8)]
        full = lambda v: jnp.full((8, LANES), v, f32)
        out = [full(ok[0]), full(ok[1])] * 3 + [full(ok[2])] * 2 + [full(ok[3])] * 2 + [full(ok[2]), full(ok[3])]
        k = full(ok[7])
        for j in (2, 1, 0):
            k = jnp.where(sub < 2 * (j + 1), full(ok[4 + j]), k)
        return out + [k]

    def ring(t, between):
        mask = ring_mask()
        for c in range(CH):
            parts = [lhs_ring[kc, tap] for kc in range(CH) for tap in range(TAPS)]
            gates = jnp.dot(
                jnp.concatenate(parts, axis=1), w[c].reshape(KDIM, 4 * LANES), preferred_element_type=f32
            )
            if c == 0:
                between()
            h, cn = lstm(gates, bias_of(t, c), c_ring[c])
            c_ring[c] = cn
            hf = h.astype(f32)
            put_ring(grid.at[c], [hf[8 * k : 8 * k + 8] * m for k, m in enumerate(mask)])
            build_border(c)

    def put_new():
        for c in range(CH):
            h = h_new[c]
            put_cells(h_dma, c, h)
            pt[c, 1:7, 1:4] = h.reshape(6, 3, 16, LANES)

    def wait_put(slot):
        for d in range(8):
            message(d, slot, True).wait_send()
        h_out(STEPS - 1).wait()

    def begin(t):
        own(t, 0)
        own(t, 1)
        own(t, 2, 0, 3)

    def step(t, carry):
        wait_put(lax.rem(t, SLOTS))
        take(lax.rem(t, SLOTS))
        for kc in range(CH):
            for tap in range(TAPS):
                v = ring_rows(grid.at[kc], tap // 3 - 1, tap % 3 - 1)
                lhs_ring[kc, tap] = jnp.concatenate(v, axis=0).astype(bf16)
        own(t, 2, 3, 6)
        put_new()

        def send():
            for d in range(8):
                message(d, lax.rem(t + 1, SLOTS), True).start()
            h_out(t).start()
            for c in range(CH):
                put_own(grid.at[c], h_new[c].astype(f32))

        ring(t, send)
        begin(t + 1)
        return carry

    w_wait(0)
    w_wait(1)
    w_wait(2)
    begin(0)
    for d in range(8):
        first_message(d, 1, False).wait_send()
    take_first(1, cgrid, firstc_v, firstc_h, firstc_k)
    for c in range(CH):
        c_ring[c] = jnp.concatenate(ring_rows(cgrid.at[c], 0, 0), axis=0)

    lax.fori_loop(0, STEPS - 1, step, 0)
    wait_put((STEPS - 1) % SLOTS)
    own(STEPS - 1, 2, 3, 6)
    put_new()
    h_out(STEPS - 1).start()
    for c in range(CH):
        put_cells(c_dma, c, c_own[c])
    c_out.start()
    for d in range(8):
        message(d, (STEPS - 1) % SLOTS, False).wait_recv()
    h_out(STEPS - 1).wait()
    c_out.wait()


def copy_out(h, c, h_out, c_out, hv, cv, in_sem, out_sem):
    pieces = [(h.at[t], hv.at[t], h_out.at[t]) for t in range(STEPS)] + [(c, cv, c_out)]
    ins = [pltpu.make_async_copy(a, v, in_sem.at[k]) for k, (a, v, b) in enumerate(pieces)]
    outs = [pltpu.make_async_copy(v, b, out_sem) for a, v, b in pieces]
    for m in ins:
        m.start()
    for m, n in zip(ins, outs):
        m.wait()
        n.start()
    for n in outs:
        n.wait()


def solution(mesh):
    def device_fn(h_init, c_init, w_rec, gate_bias):
        hbm = pl.BlockSpec(memory_space=pl.ANY)
        bf16, f32 = jnp.bfloat16, jnp.float32
        dma = pltpu.SemaphoreType.DMA
        tiles = (2, 6, 4, 3, S, CDIM)
        outs = (jax.ShapeDtypeStruct((STEPS,) + tiles, bf16), jax.ShapeDtypeStruct(tiles, f32))
        state = pl.pallas_call(
            kernel,
            out_shape=outs,
            in_specs=[hbm] * 4,
            out_specs=(hbm, hbm),
            scratch_shapes=[
                pltpu.VMEM((CH, CH, 3, 3, LANES, 4 * LANES), bf16),
                pltpu.VMEM((4 * CH, STEPS, LANES), f32),
                pltpu.VMEM((CH, 8, 5, 16, LANES), bf16),
                pltpu.VMEM((CH, GROWS, LANES), f32),
                pltpu.VMEM((CH, GROWS, LANES), f32),
                pltpu.VMEM((CH, S * T * T, LANES), bf16),
                pltpu.VMEM(tiles, bf16),
                pltpu.VMEM((CH, S * T * T, LANES), f32),
                pltpu.VMEM(tiles, f32),
                pltpu.VMEM((CH, RTILES * 16, LANES), f32),
                pltpu.VMEM((CH, TAPS, RTILES * 16, LANES), bf16),
                pltpu.VMEM((SLOTS, 2, 4, 3, S, CDIM), bf16),
                pltpu.VMEM((SLOTS, 2, 2, 6, S, CDIM), bf16),
                pltpu.VMEM((SLOTS, 4, 2, 2, S, CDIM), bf16),
                pltpu.VMEM((2, 4, 3, S, CDIM), bf16),
                pltpu.VMEM((2, 2, 6, S, CDIM), bf16),
                pltpu.VMEM((4, 1, 1, S, CDIM), bf16),
                pltpu.VMEM((2, 4, 3, S, CDIM), f32),
                pltpu.VMEM((2, 2, 6, S, CDIM), f32),
                pltpu.VMEM((4, 1, 1, S, CDIM), f32),
                dma((CH,)),
                dma((3,)),
                dma,
                dma((8,)),
                dma((SLOTS, 8)),
                dma((2, 8)),
                dma((2, 8)),
            ],
            compiler_params=pltpu.CompilerParams(
                collective_id=0, has_side_effects=True, vmem_limit_bytes=60 * 1024 * 1024
            ),
        )(
            h_init.transpose(1, 2, 0, 3).reshape(tiles),
            c_init.transpose(1, 2, 0, 3).reshape(tiles),
            w_rec,
            gate_bias,
        )
        h_seq, c_last = pl.pallas_call(
            copy_out,
            out_shape=outs,
            in_specs=[hbm] * 2,
            out_specs=(hbm, hbm),
            scratch_shapes=[
                pltpu.VMEM((STEPS,) + tiles, bf16),
                pltpu.VMEM(tiles, f32),
                dma((STEPS + 1,)),
                dma,
            ],
        )(*state)
        h_seq = h_seq.reshape(STEPS, T, T, S, CDIM).transpose(0, 3, 1, 2, 4)
        return h_seq, c_last.reshape(T, T, S, CDIM).transpose(2, 0, 1, 3)

    state_spec = P("dp", "rows", "cols", None)
    return jax.shard_map(
        device_fn,
        mesh=mesh,
        in_specs=(state_spec, state_spec, P(), P()),
        out_specs=(P(None, "dp", "rows", "cols", None), state_spec),
        check_vma=False,
    )
```

```python
import jax
import jax.numpy as jnp
from jax import lax
from jax.experimental import pallas as pl
from jax.experimental.pallas import tpu as pltpu
from jax.sharding import PartitionSpec as P

MESH = pl.DeviceIdType.MESH
STEPS = 12
S = 2
T = 12
LANES = 128
CH = 3
CDIM = CH * LANES
TAPS = 9
KDIM = TAPS * CDIM
SLOTS = 4

YPITCH = 3 * 6 * S
GROWS = 20 * YPITCH
RTILES = 7

DIRS = ((-1, 0), (1, 0), (0, -1), (0, 1), (-1, -1), (-1, 1), (1, -1), (1, 1))


def opposite(d):
    dy, dx = DIRS[d]
    return DIRS.index((-dy, -dx))


def at(y, x):
    return ((y + 2) * 3 + (x + 2) % 3) * 6 * S + (x + 2) // 3 * S


def sigmoid(v):
    return 0.5 * jnp.tanh(0.5 * v) + 0.5


def lstm(gates, bias, c_prev):
    i, f, o, g = (gates[:, k * LANES : (k + 1) * LANES] + bias[k] for k in range(4))
    c = sigmoid(f) * c_prev + sigmoid(i) * jnp.tanh(g)
    h = (sigmoid(o) * jnp.tanh(c)).astype(jnp.bfloat16)
    return h, c


def side_rows(dy):
    return -1 if dy < 0 else T


def ring_rows(g, dy, dx):
    sub = lax.broadcasted_iota(jnp.int32, (8, LANES), 0)
    out = []
    for ix in range(3):
        for y in (-1, T):
            out.append(g[pl.ds(at(y + dy, ix + dx), 8), :])
    for x in (-1, T):
        for s in range(S):
            out.append(g[pl.ds(at(dy, x + dx) + s, 8, stride=YPITCH), :])
    for x in (-1, T):
        a = g[pl.ds(at(8 + dy, x + dx), 8, stride=YPITCH), :]
        b = g[pl.ds(at(4 + dy, x + dx) + 1, 8, stride=YPITCH), :]
        out.append(jnp.where(sub < 4, a, b))
    v = None
    for k, (y, x) in enumerate(((-1, -1), (-1, T), (T, -1), (T, T))):
        a = g[pl.ds(at(y + dy, x + dx) - 2 * k, 8), :]
        v = a if v is None else jnp.where(sub < 2 * k, v, a)
    return out + [v, v]


def put_ring(g, v):
    k = 0
    for ix in range(3):
        for y in (-1, T):
            g[pl.ds(at(y, ix), 8), :] = v[k]
            k += 1
    for x in (-1, T):
        for s in range(S):
            g[pl.ds(at(0, x) + s, 8, stride=YPITCH), :] = v[k]
            k += 1
    for x in (-1, T):
        for s in range(S):
            g[pl.ds(at(8, x) + s, 4, stride=YPITCH), :] = v[k][4 * s : 4 * s + 4]
        k += 1
    for j, (y, x) in enumerate(((-1, -1), (-1, T), (T, -1), (T, T))):
        g[pl.ds(at(y, x), 2), :] = v[k][2 * j : 2 * j + 2]


def lanes(c):
    return slice(c * LANES, (c + 1) * LANES)


def line_pieces(line, c):
    if line.shape[0] == 4:
        return [line[:, ix, :, lanes(c)].reshape(8, LANES) for ix in range(3)]
    return [line[jy, :, :, lanes(c)].reshape(12, LANES) for jy in range(2)]


def put_line(g, d, dist, pieces):
    dy, dx = DIRS[d]
    if dx == 0:
        y = -dist if dy < 0 else T - 1 + dist
        for ix in range(3):
            g[pl.ds(at(y, ix), 8), :] = pieces[ix]
    else:
        x = -dist if dx < 0 else T - 1 + dist
        for jy in range(2):
            for iy in range(6):
                g[pl.ds(at(6 * jy + iy, x), 2), :] = pieces[jy][2 * iy : 2 * iy + 2]


def put_cells(ref, c, v):
    k = 0
    for iy in range(6):
        for ix in range(3):
            for jy in range(2):
                ref[jy, iy, :, ix, :, lanes(c)] = v[k : k + 8].reshape(4, S, LANES)
                k += 8


def get_cells(ref, c):
    return jnp.concatenate(
        [
            ref[jy, iy, :, ix, :, lanes(c)].reshape(8, LANES)
            for iy in range(6)
            for ix in range(3)
            for jy in range(2)
        ],
        axis=0,
    )


def kernel(
    h_hbm, c_hbm, w_hbm, bias_hbm, h_seq, c_last,
    h_init, c_init, w, bias, pt, grid, cgrid, h_new, half, c_own, c_ring, lhs_ring,
    recv_v, recv_h, recv_k, first_v, first_h, first_k, firstc_v, firstc_h, firstc_k,
    w_sem, bias_sem, in_sem, send_sem, recv_sem, fsend_sem, frecv_sem,
):
    rows_n, cols_n = lax.axis_size("rows"), lax.axis_size("cols")
    my_row, my_col = lax.axis_index("rows"), lax.axis_index("cols")
    f32, bf16 = jnp.float32, jnp.bfloat16

    def lacks(d):
        dy, dx = DIRS[d]
        r = jnp.bool_(False) if dy == 0 else my_row == (0 if dy < 0 else rows_n - 1)
        c = jnp.bool_(False) if dx == 0 else my_col == (0 if dx < 0 else cols_n - 1)
        return r, c, jnp.logical_or(r, c)

    def flip(v):
        return v + 1 - 2 * lax.rem(v, 2)

    def peer(d, back):
        dy, dx = DIRS[d]
        lr, lc, lack = lacks(d)
        if dx == 0:
            r, c = my_row, flip(my_col)
        elif dy == 0:
            r, c = flip(my_row), my_col
        else:
            a = my_row if dy < 0 else rows_n - 1 - my_row
            b = my_col if dx < 0 else cols_n - 1 - my_col
            on_c = jnp.logical_and(lc, a >= 2)
            on_r = jnp.logical_and(lr, b >= 2)
            if back:
                a3, b3 = jnp.where(a == 1, 0, jnp.where(b == 1, 0, 1)), jnp.where(a == 1, 1, 0)
            else:
                a3, b3 = jnp.where(b == 1, 1, 0), jnp.where(jnp.logical_and(a == 0, b == 0), 1, 0)
            a2 = jnp.where(on_c, flip(a), jnp.where(on_r, 0, a3))
            b2 = jnp.where(on_c, 0, jnp.where(on_r, flip(b), b3))
            r = a2 if dy < 0 else rows_n - 1 - a2
            c = b2 if dx < 0 else cols_n - 1 - b2
        return {"rows": jnp.where(lack, r, my_row + dy), "cols": jnp.where(lack, c, my_col + dx)}

    lack = [lacks(d)[2] for d in range(8)]
    peers = [peer(d, False) for d in range(8)]
    landing = [jnp.where(lack[d], d, opposite(d)) for d in range(8)]

    def kept(d, v):
        return jnp.where(lack[d], jnp.zeros_like(v), v)

    def edge_cells(d, depth):
        dy, dx = DIRS[d]
        every = slice(None)
        if dx == 0:
            return (0, depth, every, every) if dy < 0 else (1, 5 - depth, every, every)
        return (every, every, 0, depth) if dx < 0 else (every, every, 3, 2 - depth)

    def corner_cells(d, n):
        dy, dx = DIRS[d]
        jy, iy = (0, slice(0, n)) if dy < 0 else (1, slice(6 - n, 6))
        jx, ix = (0, slice(0, n)) if dx < 0 else (3, slice(3 - n, 3))
        return jy, iy, jx, ix

    def remote(d, src, dst, dst_back, ssem, rsem, rsem_back, sending):
        return pltpu.make_async_remote_copy(
            src_ref=src, dst_ref=dst if sending else dst_back,
            send_sem=ssem, recv_sem=rsem if sending else rsem_back,
            device_id=peers[d], device_id_type=MESH,
        )

    def message(d, slot, sending, h):
        e = landing[d]
        if d < 2:
            src, dst = h.at[edge_cells(d, 1)], lambda k: recv_v.at[slot, k]
        elif d < 4:
            src, dst = h.at[edge_cells(d, 1)], lambda k: recv_h.at[slot, k - 2]
        else:
            src, dst = h.at[corner_cells(d, 2)], lambda k: recv_k.at[slot, k - 4]
        return remote(
            d, src, dst(e), dst(d), send_sem.at[d], recv_sem.at[slot, e], recv_sem.at[slot, d], sending
        )

    def first_message(d, k, sending):
        e = landing[d]
        cells = edge_cells(d, 0) if d < 4 else corner_cells(d, 1)
        src = (c_init if k else h_init).at[cells]
        if d < 2:
            dst = lambda j: (firstc_v if k else first_v).at[j]
        elif d < 4:
            dst = lambda j: (firstc_h if k else first_h).at[j - 2]
        else:
            dst = lambda j: (firstc_k if k else first_k).at[j - 4]
        return remote(
            d, src, dst(e), dst(d), fsend_sem.at[k, d], frecv_sem.at[k, e], frecv_sem.at[k, d], sending
        )

    h_in = pltpu.make_async_copy(h_hbm, h_init, in_sem.at[0])
    c_in = pltpu.make_async_copy(c_hbm, c_init, in_sem.at[1])
    h_in.start()
    c_in.start()
    barrier = pltpu.get_barrier_semaphore()
    for d in range(8):
        pl.semaphore_signal(barrier, inc=1, device_id=peer(d, True), device_id_type=MESH)

    bias_copies = [
        pltpu.make_async_copy(bias_hbm.at[:, pl.ds(k * LANES, LANES)], bias.at[k], bias_sem) for k in range(4 * CH)
    ]
    for m in bias_copies:
        m.start()
    for c in range(CH):
        for kc in range(CH):
            for g in range(4):
                pltpu.make_async_copy(
                    w_hbm.at[:, :, pl.ds(kc * LANES, LANES), pl.ds(g * CDIM + c * LANES, LANES)],
                    w.at[c, kc, :, :, :, pl.ds(g * LANES, LANES)],
                    w_sem.at[c],
                ).start()

    def w_wait(c):
        pltpu.make_async_copy(w.at[c], w.at[c], w_sem.at[c]).wait()

    h_in.wait()
    pl.semaphore_wait(barrier, 8)
    for d in range(8):
        first_message(d, 0, True).start()
    for d in range(8):
        message(d, 0, True, h_init).start()
    c_in.wait()
    for d in range(8):
        first_message(d, 1, True).start()
    for c in range(CH):
        c_own[c] = get_cells(c_init, c)

    def put_own(g, hf):
        k = 0
        for iy in range(6):
            for ix in range(3):
                for jy in range(2):
                    g[pl.ds(at(6 * jy + iy, ix), 8), :] = hf[k : k + 8]
                    k += 8

    for c in range(CH):
        h = get_cells(h_init, c)
        pt[c, 1:7, 1:4] = h.reshape(6, 3, 16, LANES)
        put_own(grid.at[c], h.astype(f32))

    def take_first(k, to, gv, gh, gk):
        for d in range(8):
            first_message(d, k, False).wait_recv()
        for c in range(CH):
            g = to.at[c]
            for d in range(4):
                v = line_pieces((gv if d < 2 else gh).at[d % 2], c)
                put_line(g, d, 1, [kept(d, a.astype(f32)) for a in v])
            for d in range(4, 8):
                v = gk[d - 4, 0, 0, :, lanes(c)].astype(f32)
                dy, dx = DIRS[d]
                g[pl.ds(at(side_rows(dy), side_rows(dx)), 2), :] = kept(d, v)

    def build_border(c):
        g = grid.at[c]
        for ty in range(-1, 7):
            for tx in range(-1, 4):
                if not (0 <= ty < 6 and 0 <= tx < 3):
                    v = jnp.concatenate([g[pl.ds(at(ty + 6 * jy, tx), 8), :] for jy in range(2)], axis=0)
                    pt[c, ty + 1, tx + 1] = v.astype(bf16)

    take_first(0, grid, first_v, first_h, first_k)
    for d in range(8):
        first_message(d, 0, False).wait_send()
    for c in range(CH):
        build_border(c)
    for m in bias_copies:
        m.wait()

    def bias_of(t, c):
        return [bias[g * CH + c, pl.ds(t, 1), :] for g in range(4)]

    def own_gates(c, lo, hi):
        parts = [
            pt[kc, lo + tap // 3 : hi + tap // 3, tap % 3 : tap % 3 + 3].reshape((hi - lo) * 48, LANES)
            for kc in range(CH)
            for tap in range(TAPS)
        ]
        return jnp.dot(
            jnp.concatenate(parts, axis=1), w[c].reshape(KDIM, 4 * LANES), preferred_element_type=f32
        )

    def own_update(t, c, lo, hi, gates):
        rows = pl.ds(lo * 48, (hi - lo) * 48)
        h, cn = lstm(gates, bias_of(t, c), c_own[c, rows])
        c_own[c, rows] = cn
        h_new[c, rows] = h

    def take(slot):
        for d in range(8):
            message(d, slot, False, h_init).wait_recv()
        for c in range(CH):
            g = grid.at[c]
            for d in range(4):
                v = line_pieces((recv_v if d < 2 else recv_h).at[slot, d % 2], c)
                put_line(g, d, 2, [kept(d, a.astype(f32)) for a in v])
            for d in range(4, 8):
                v = kept(d, recv_k[slot, d - 4, :, :, :, lanes(c)].reshape(8, LANES).astype(f32))
                dy, dx = DIRS[d]
                y0, x0 = (-2 if dy < 0 else T), (-2 if dx < 0 else T)
                for k in range(4):
                    y, x = y0 + k // 2, x0 + k % 2
                    if (y, x) != (side_rows(dy), side_rows(dx)):
                        g[pl.ds(at(y, x), 2), :] = v[2 * k : 2 * k + 2]

    def ring_mask():
        sub = lax.broadcasted_iota(jnp.int32, (8, LANES), 0)
        ok = [jnp.where(lack[d], 0.0, 1.0).astype(f32) for d in range(8)]
        full = lambda v: jnp.full((8, LANES), v, f32)
        out = [full(ok[0]), full(ok[1])] * 3 + [full(ok[2])] * 2 + [full(ok[3])] * 2 + [full(ok[2]), full(ok[3])]
        k = full(ok[7])
        for j in (2, 1, 0):
            k = jnp.where(sub < 2 * (j + 1), full(ok[4 + j]), k)
        return out + [k]

    def ring(t, between):
        mask = ring_mask()
        for c in range(CH):
            parts = [lhs_ring[kc, tap] for kc in range(CH) for tap in range(TAPS)]
            gates = jnp.dot(
                jnp.concatenate(parts, axis=1), w[c].reshape(KDIM, 4 * LANES), preferred_element_type=f32
            )
            if c == 0:
                between()
            h, cn = lstm(gates, bias_of(t, c), c_ring[c])
            c_ring[c] = cn
            hf = h.astype(f32)
            put_ring(grid.at[c], [hf[8 * k : 8 * k + 8] * m for k, m in enumerate(mask)])
            build_border(c)

    def put_new(t):
        for c in range(CH):
            h = h_new[c]
            put_cells(h_seq.at[t], c, h)
            pt[c, 1:7, 1:4] = h.reshape(6, 3, 16, LANES)

    def begin(t):
        for c in range(2):
            own_update(t, c, 0, 6, own_gates(c, 0, 6))
        half[...] = own_gates(2, 0, 3)

    def finish(t):
        own_update(t, 2, 0, 3, half[...])
        own_update(t, 2, 3, 6, own_gates(2, 3, 6))
        put_new(t)

    def sent(slot):
        for d in range(8):
            message(d, slot, True, h_init).wait_send()

    def step(t, carry):
        sent(lax.rem(t, SLOTS))
        take(lax.rem(t, SLOTS))
        for kc in range(CH):
            for tap in range(TAPS):
                v = ring_rows(grid.at[kc], tap // 3 - 1, tap % 3 - 1)
                lhs_ring[kc, tap] = jnp.concatenate(v, axis=0).astype(bf16)
        finish(t)

        def send():
            for d in range(8):
                message(d, lax.rem(t + 1, SLOTS), True, h_seq.at[t]).start()
            for c in range(CH):
                put_own(grid.at[c], h_new[c].astype(f32))

        ring(t, send)
        begin(t + 1)
        return carry

    w_wait(0)
    w_wait(1)
    w_wait(2)
    begin(0)
    for d in range(8):
        first_message(d, 1, False).wait_send()
    take_first(1, cgrid, firstc_v, firstc_h, firstc_k)
    for c in range(CH):
        c_ring[c] = jnp.concatenate(ring_rows(cgrid.at[c], 0, 0), axis=0)

    lax.fori_loop(0, STEPS - 1, step, 0)
    sent((STEPS - 1) % SLOTS)
    for d in range(8):
        message(d, (STEPS - 1) % SLOTS, False, h_init).wait_recv()
    finish(STEPS - 1)
    for c in range(CH):
        put_cells(c_last, c, c_own[c])


def copy_out(h, c, h_out, c_out, sem):
    copies = [pltpu.make_async_copy(h, h_out, sem.at[0]), pltpu.make_async_copy(c, c_out, sem.at[1])]
    for m in copies:
        m.start()
    for m in copies:
        m.wait()


def solution(mesh):
    def device_fn(h_init, c_init, w_rec, gate_bias):
        hbm = pl.BlockSpec(memory_space=pl.ANY)
        vmem = pl.BlockSpec(memory_space=pltpu.VMEM)
        bf16, f32 = jnp.bfloat16, jnp.float32
        dma = pltpu.SemaphoreType.DMA
        tiles = (2, 6, 4, 3, S, CDIM)
        outs = (jax.ShapeDtypeStruct((STEPS,) + tiles, bf16), jax.ShapeDtypeStruct(tiles, f32))
        state = pl.pallas_call(
            kernel,
            out_shape=tuple(pltpu.VMEM(o.shape, o.dtype) for o in outs),
            in_specs=[hbm] * 4,
            out_specs=(vmem, vmem),
            scratch_shapes=[
                pltpu.VMEM(tiles, bf16),
                pltpu.VMEM(tiles, f32),
                pltpu.VMEM((CH, CH, 3, 3, LANES, 4 * LANES), bf16),
                pltpu.VMEM((4 * CH, STEPS, LANES), f32),
                pltpu.VMEM((CH, 8, 5, 16, LANES), bf16),
                pltpu.VMEM((CH, GROWS, LANES), f32),
                pltpu.VMEM((CH, GROWS, LANES), f32),
                pltpu.VMEM((CH, S * T * T, LANES), bf16),
                pltpu.VMEM((S * T * T // 2, 4 * LANES), f32),
                pltpu.VMEM((CH, S * T * T, LANES), f32),
                pltpu.VMEM((CH, RTILES * 16, LANES), f32),
                pltpu.VMEM((CH, TAPS, RTILES * 16, LANES), bf16),
                pltpu.VMEM((SLOTS, 2, 4, 3, S, CDIM), bf16),
                pltpu.VMEM((SLOTS, 2, 2, 6, S, CDIM), bf16),
                pltpu.VMEM((SLOTS, 4, 2, 2, S, CDIM), bf16),
                pltpu.VMEM((2, 4, 3, S, CDIM), bf16),
                pltpu.VMEM((2, 2, 6, S, CDIM), bf16),
                pltpu.VMEM((4, 1, 1, S, CDIM), bf16),
                pltpu.VMEM((2, 4, 3, S, CDIM), f32),
                pltpu.VMEM((2, 2, 6, S, CDIM), f32),
                pltpu.VMEM((4, 1, 1, S, CDIM), f32),
                dma((CH,)),
                dma,
                dma((2,)),
                dma((8,)),
                dma((SLOTS, 8)),
                dma((2, 8)),
                dma((2, 8)),
            ],
            compiler_params=pltpu.CompilerParams(
                collective_id=0, has_side_effects=True, vmem_limit_bytes=58 * 1024 * 1024
            ),
        )(
            h_init.transpose(1, 2, 0, 3).reshape(tiles),
            c_init.transpose(1, 2, 0, 3).reshape(tiles),
            w_rec,
            gate_bias,
        )
        h_seq, c_last = pl.pallas_call(
            copy_out,
            out_shape=outs,
            in_specs=[vmem] * 2,
            out_specs=(hbm, hbm),
            scratch_shapes=[dma((2,))],
            compiler_params=pltpu.CompilerParams(vmem_limit_bytes=16 * 1024 * 1024),
        )(*state)
        h_seq = h_seq.reshape(STEPS, T, T, S, CDIM).transpose(0, 3, 1, 2, 4)
        return h_seq, c_last.reshape(T, T, S, CDIM).transpose(2, 0, 1, 3)

    state_spec = P("dp", "rows", "cols", None)
    return jax.shard_map(
        device_fn,
        mesh=mesh,
        in_specs=(state_spec, state_spec, P(), P()),
        out_specs=(P(None, "dp", "rows", "cols", None), state_spec),
        check_vma=False,
    )
```

```python
import jax
import jax.numpy as jnp
from jax import lax
from jax.experimental import pallas as pl
from jax.experimental.pallas import tpu as pltpu
from jax.sharding import PartitionSpec as P

MESH = pl.DeviceIdType.MESH
STEPS = 12
S = 2
T = 12
LANES = 128
CH = 3
CDIM = CH * LANES
TAPS = 9
KDIM = TAPS * CDIM
SLOTS = 4

YPITCH = 3 * 6 * S
GROWS = 20 * YPITCH
RTILES = 7

DIRS = ((-1, 0), (1, 0), (0, -1), (0, 1), (-1, -1), (-1, 1), (1, -1), (1, 1))


def opposite(d):
    dy, dx = DIRS[d]
    return DIRS.index((-dy, -dx))


def at(y, x):
    return ((y + 2) * 3 + (x + 2) % 3) * 6 * S + (x + 2) // 3 * S


def sigmoid(v):
    return 0.5 * jnp.tanh(0.5 * v) + 0.5


def lstm(gates, bias, c_prev):
    i, f, o, g = (gates[:, k * LANES : (k + 1) * LANES] + bias[k] for k in range(4))
    c = sigmoid(f) * c_prev + sigmoid(i) * jnp.tanh(g)
    h = (sigmoid(o) * jnp.tanh(c)).astype(jnp.bfloat16)
    return h, c


def side_rows(dy):
    return -1 if dy < 0 else T


def ring_rows(g, dy, dx):
    sub = lax.broadcasted_iota(jnp.int32, (8, LANES), 0)
    out = []
    for ix in range(3):
        for y in (-1, T):
            out.append(g[pl.ds(at(y + dy, ix + dx), 8), :])
    for x in (-1, T):
        for s in range(S):
            out.append(g[pl.ds(at(dy, x + dx) + s, 8, stride=YPITCH), :])
    for x in (-1, T):
        a = g[pl.ds(at(8 + dy, x + dx), 8, stride=YPITCH), :]
        b = g[pl.ds(at(4 + dy, x + dx) + 1, 8, stride=YPITCH), :]
        out.append(jnp.where(sub < 4, a, b))
    v = None
    for k, (y, x) in enumerate(((-1, -1), (-1, T), (T, -1), (T, T))):
        a = g[pl.ds(at(y + dy, x + dx) - 2 * k, 8), :]
        v = a if v is None else jnp.where(sub < 2 * k, v, a)
    return out + [v, v]


def put_ring(g, v):
    k = 0
    for ix in range(3):
        for y in (-1, T):
            g[pl.ds(at(y, ix), 8), :] = v[k]
            k += 1
    for x in (-1, T):
        for s in range(S):
            g[pl.ds(at(0, x) + s, 8, stride=YPITCH), :] = v[k]
            k += 1
    for x in (-1, T):
        for s in range(S):
            g[pl.ds(at(8, x) + s, 4, stride=YPITCH), :] = v[k][4 * s : 4 * s + 4]
        k += 1
    for j, (y, x) in enumerate(((-1, -1), (-1, T), (T, -1), (T, T))):
        g[pl.ds(at(y, x), 2), :] = v[k][2 * j : 2 * j + 2]


def lanes(c):
    return slice(c * LANES, (c + 1) * LANES)


def line_pieces(line, c):
    if line.shape[0] == 4:
        return [line[:, ix, :, lanes(c)].reshape(8, LANES) for ix in range(3)]
    return [line[jy, :, :, lanes(c)].reshape(12, LANES) for jy in range(2)]


def put_line(g, d, dist, pieces):
    dy, dx = DIRS[d]
    if dx == 0:
        y = -dist if dy < 0 else T - 1 + dist
        for ix in range(3):
            g[pl.ds(at(y, ix), 8), :] = pieces[ix]
    else:
        x = -dist if dx < 0 else T - 1 + dist
        for jy in range(2):
            for iy in range(6):
                g[pl.ds(at(6 * jy + iy, x), 2), :] = pieces[jy][2 * iy : 2 * iy + 2]


def put_cells(ref, c, v):
    k = 0
    for iy in range(6):
        for ix in range(3):
            for jy in range(2):
                ref[jy, iy, :, ix, :, lanes(c)] = v[k : k + 8].reshape(4, S, LANES)
                k += 8


def get_cells(ref, c):
    return jnp.concatenate(
        [
            ref[jy, iy, :, ix, :, lanes(c)].reshape(8, LANES)
            for iy in range(6)
            for ix in range(3)
            for jy in range(2)
        ],
        axis=0,
    )


def kernel(
    h_hbm, c_hbm, w_hbm, bias_hbm, h_seq, c_last,
    h_init, c_init, w, bias, pt, grid, cgrid, h_new, half, c_own, c_ring, lhs_ring,
    recv_v, recv_h, recv_k, first_v, first_h, first_k, firstc_v, firstc_h, firstc_k,
    w_sem, bias_sem, in_sem, send_sem, recv_sem, fsend_sem, frecv_sem,
):
    rows_n, cols_n = lax.axis_size("rows"), lax.axis_size("cols")
    my_row, my_col = lax.axis_index("rows"), lax.axis_index("cols")
    f32, bf16 = jnp.float32, jnp.bfloat16

    def lacks(d):
        dy, dx = DIRS[d]
        r = jnp.bool_(False) if dy == 0 else my_row == (0 if dy < 0 else rows_n - 1)
        c = jnp.bool_(False) if dx == 0 else my_col == (0 if dx < 0 else cols_n - 1)
        return r, c, jnp.logical_or(r, c)

    def flip(v):
        return v + 1 - 2 * lax.rem(v, 2)

    def peer(d, back):
        dy, dx = DIRS[d]
        lr, lc, lack = lacks(d)
        if dx == 0:
            r, c = my_row, flip(my_col)
        elif dy == 0:
            r, c = flip(my_row), my_col
        else:
            a = my_row if dy < 0 else rows_n - 1 - my_row
            b = my_col if dx < 0 else cols_n - 1 - my_col
            on_c = jnp.logical_and(lc, a >= 2)
            on_r = jnp.logical_and(lr, b >= 2)
            if back:
                a3, b3 = jnp.where(a == 1, 0, jnp.where(b == 1, 0, 1)), jnp.where(a == 1, 1, 0)
            else:
                a3, b3 = jnp.where(b == 1, 1, 0), jnp.where(jnp.logical_and(a == 0, b == 0), 1, 0)
            a2 = jnp.where(on_c, flip(a), jnp.where(on_r, 0, a3))
            b2 = jnp.where(on_c, 0, jnp.where(on_r, flip(b), b3))
            r = a2 if dy < 0 else rows_n - 1 - a2
            c = b2 if dx < 0 else cols_n - 1 - b2
        return {"rows": jnp.where(lack, r, my_row + dy), "cols": jnp.where(lack, c, my_col + dx)}

    lack = [lacks(d)[2] for d in range(8)]
    peers = [peer(d, False) for d in range(8)]
    landing = [jnp.where(lack[d], d, opposite(d)) for d in range(8)]

    def kept(d, v):
        return jnp.where(lack[d], jnp.zeros_like(v), v)

    def edge_cells(d, depth):
        dy, dx = DIRS[d]
        every = slice(None)
        if dx == 0:
            return (0, depth, every, every) if dy < 0 else (1, 5 - depth, every, every)
        return (every, every, 0, depth) if dx < 0 else (every, every, 3, 2 - depth)

    def corner_cells(d, n):
        dy, dx = DIRS[d]
        jy, iy = (0, slice(0, n)) if dy < 0 else (1, slice(6 - n, 6))
        jx, ix = (0, slice(0, n)) if dx < 0 else (3, slice(3 - n, 3))
        return jy, iy, jx, ix

    def remote(d, src, dst, dst_back, ssem, rsem, rsem_back, sending):
        return pltpu.make_async_remote_copy(
            src_ref=src, dst_ref=dst if sending else dst_back,
            send_sem=ssem, recv_sem=rsem if sending else rsem_back,
            device_id=peers[d], device_id_type=MESH,
        )

    def message(d, slot, sending, h):
        e = landing[d]
        if d < 2:
            src, dst = h.at[edge_cells(d, 1)], lambda k: recv_v.at[slot, k]
        elif d < 4:
            src, dst = h.at[edge_cells(d, 1)], lambda k: recv_h.at[slot, k - 2]
        else:
            src, dst = h.at[corner_cells(d, 2)], lambda k: recv_k.at[slot, k - 4]
        return remote(
            d, src, dst(e), dst(d), send_sem.at[d], recv_sem.at[slot, e], recv_sem.at[slot, d], sending
        )

    def first_message(d, k, sending):
        e = landing[d]
        cells = edge_cells(d, 0) if d < 4 else corner_cells(d, 1)
        src = (c_init if k else h_init).at[cells]
        if d < 2:
            dst = lambda j: (firstc_v if k else first_v).at[j]
        elif d < 4:
            dst = lambda j: (firstc_h if k else first_h).at[j - 2]
        else:
            dst = lambda j: (firstc_k if k else first_k).at[j - 4]
        return remote(
            d, src, dst(e), dst(d), fsend_sem.at[k, d], frecv_sem.at[k, e], frecv_sem.at[k, d], sending
        )

    h_in = pltpu.make_async_copy(h_hbm, h_init, in_sem.at[0])
    c_in = pltpu.make_async_copy(c_hbm, c_init, in_sem.at[1])
    h_in.start()
    c_in.start()
    barrier = pltpu.get_barrier_semaphore()
    for d in range(8):
        pl.semaphore_signal(barrier, inc=1, device_id=peer(d, True), device_id_type=MESH)

    bias_copies = [
        pltpu.make_async_copy(bias_hbm.at[:, pl.ds(k * LANES, LANES)], bias.at[k], bias_sem) for k in range(4 * CH)
    ]
    for m in bias_copies:
        m.start()
    for c in range(CH):
        for kc in range(CH):
            for g in range(4):
                pltpu.make_async_copy(
                    w_hbm.at[:, :, pl.ds(kc * LANES, LANES), pl.ds(g * CDIM + c * LANES, LANES)],
                    w.at[c, kc, :, :, :, pl.ds(g * LANES, LANES)],
                    w_sem.at[c],
                ).start()

    def w_wait(c):
        pltpu.make_async_copy(w.at[c], w.at[c], w_sem.at[c]).wait()

    h_in.wait()
    pl.semaphore_wait(barrier, 8)
    for d in range(8):
        first_message(d, 0, True).start()
    for d in range(8):
        message(d, 0, True, h_init).start()
    c_in.wait()
    for d in range(8):
        first_message(d, 1, True).start()
    for c in range(CH):
        c_own[c] = get_cells(c_init, c)

    def put_own(g, hf):
        k = 0
        for iy in range(6):
            for ix in range(3):
                for jy in range(2):
                    g[pl.ds(at(6 * jy + iy, ix), 8), :] = hf[k : k + 8]
                    k += 8

    for c in range(CH):
        h = get_cells(h_init, c)
        pt[c, 1:7, 1:4] = h.reshape(6, 3, 16, LANES)
        put_own(grid.at[c], h.astype(f32))

    def take_first(k, to, gv, gh, gk):
        for d in range(8):
            first_message(d, k, False).wait_recv()
        for c in range(CH):
            g = to.at[c]
            for d in range(4):
                v = line_pieces((gv if d < 2 else gh).at[d % 2], c)
                put_line(g, d, 1, [kept(d, a.astype(f32)) for a in v])
            for d in range(4, 8):
                v = gk[d - 4, 0, 0, :, lanes(c)].astype(f32)
                dy, dx = DIRS[d]
                g[pl.ds(at(side_rows(dy), side_rows(dx)), 2), :] = kept(d, v)

    def build_border(c):
        g = grid.at[c]
        for ty in range(-1, 7):
            for tx in range(-1, 4):
                if not (0 <= ty < 6 and 0 <= tx < 3):
                    v = jnp.concatenate([g[pl.ds(at(ty + 6 * jy, tx), 8), :] for jy in range(2)], axis=0)
                    pt[c, ty + 1, tx + 1] = v.astype(bf16)

    take_first(0, grid, first_v, first_h, first_k)
    for d in range(8):
        first_message(d, 0, False).wait_send()
    for c in range(CH):
        build_border(c)
    for m in bias_copies:
        m.wait()

    def bias_of(t, c):
        return [bias[g * CH + c, pl.ds(t, 1), :] for g in range(4)]

    def own_gates(c, lo, hi):
        parts = [
            pt[kc, lo + tap // 3 : hi + tap // 3, tap % 3 : tap % 3 + 3].reshape((hi - lo) * 48, LANES)
            for kc in range(CH)
            for tap in range(TAPS)
        ]
        return jnp.dot(
            jnp.concatenate(parts, axis=1), w[c].reshape(KDIM, 4 * LANES), preferred_element_type=f32
        )

    def own_update(t, c, lo, hi, gates):
        rows = pl.ds(lo * 48, (hi - lo) * 48)
        h, cn = lstm(gates, bias_of(t, c), c_own[c, rows])
        c_own[c, rows] = cn
        h_new[c, rows] = h

    def take(slot):
        for d in range(8):
            message(d, slot, False, h_init).wait_recv()
        for c in range(CH):
            g = grid.at[c]
            for d in range(4):
                v = line_pieces((recv_v if d < 2 else recv_h).at[slot, d % 2], c)
                put_line(g, d, 2, [kept(d, a.astype(f32)) for a in v])
            for d in range(4, 8):
                v = kept(d, recv_k[slot, d - 4, :, :, :, lanes(c)].reshape(8, LANES).astype(f32))
                dy, dx = DIRS[d]
                y0, x0 = (-2 if dy < 0 else T), (-2 if dx < 0 else T)
                for k in range(4):
                    y, x = y0 + k // 2, x0 + k % 2
                    if (y, x) != (side_rows(dy), side_rows(dx)):
                        g[pl.ds(at(y, x), 2), :] = v[2 * k : 2 * k + 2]

    def ring_mask():
        sub = lax.broadcasted_iota(jnp.int32, (8, LANES), 0)
        ok = [jnp.where(lack[d], 0.0, 1.0).astype(f32) for d in range(8)]
        full = lambda v: jnp.full((8, LANES), v, f32)
        out = [full(ok[0]), full(ok[1])] * 3 + [full(ok[2])] * 2 + [full(ok[3])] * 2 + [full(ok[2]), full(ok[3])]
        k = full(ok[7])
        for j in (2, 1, 0):
            k = jnp.where(sub < 2 * (j + 1), full(ok[4 + j]), k)
        return out + [k]

    def ring(t, between):
        mask = ring_mask()
        for c in range(CH):
            parts = [lhs_ring[kc, tap] for kc in range(CH) for tap in range(TAPS)]
            gates = jnp.dot(
                jnp.concatenate(parts, axis=1), w[c].reshape(KDIM, 4 * LANES), preferred_element_type=f32
            )
            if c == 0:
                between()
            h, cn = lstm(gates, bias_of(t, c), c_ring[c])
            c_ring[c] = cn
            hf = h.astype(f32)
            put_ring(grid.at[c], [hf[8 * k : 8 * k + 8] * m for k, m in enumerate(mask)])
            build_border(c)

    def put_new(t):
        for c in range(CH):
            h = h_new[c]
            put_cells(h_seq.at[t], c, h)
            pt[c, 1:7, 1:4] = h.reshape(6, 3, 16, LANES)

    def begin(t):
        for c in range(2):
            own_update(t, c, 0, 6, own_gates(c, 0, 6))
        half[...] = own_gates(2, 0, 3)

    def finish(t):
        own_update(t, 2, 0, 3, half[...])
        own_update(t, 2, 3, 6, own_gates(2, 3, 6))
        put_new(t)

    def sent(slot):
        for d in range(8):
            message(d, slot, True, h_init).wait_send()

    def step(t, carry):
        sent(lax.rem(t, SLOTS))
        take(lax.rem(t, SLOTS))
        for kc in range(CH):
            for tap in range(TAPS):
                v = ring_rows(grid.at[kc], tap // 3 - 1, tap % 3 - 1)
                lhs_ring[kc, tap] = jnp.concatenate(v, axis=0).astype(bf16)
        finish(t)

        def send():
            for d in (4, 5, 6, 7, 2, 3, 0, 1):
                message(d, lax.rem(t + 1, SLOTS), True, h_seq.at[t]).start()
            for c in range(CH):
                put_own(grid.at[c], h_new[c].astype(f32))

        ring(t, send)
        begin(t + 1)
        return carry

    w_wait(0)
    w_wait(1)
    w_wait(2)
    begin(0)
    for d in range(8):
        first_message(d, 1, False).wait_send()
    take_first(1, cgrid, firstc_v, firstc_h, firstc_k)
    for c in range(CH):
        c_ring[c] = jnp.concatenate(ring_rows(cgrid.at[c], 0, 0), axis=0)

    lax.fori_loop(0, STEPS - 1, step, 0)
    sent((STEPS - 1) % SLOTS)
    for d in range(8):
        message(d, (STEPS - 1) % SLOTS, False, h_init).wait_recv()
    finish(STEPS - 1)
    for c in range(CH):
        put_cells(c_last, c, c_own[c])


def copy_out(h, c, h_out, c_out, sem):
    copies = [pltpu.make_async_copy(h, h_out, sem.at[0]), pltpu.make_async_copy(c, c_out, sem.at[1])]
    for m in copies:
        m.start()
    for m in copies:
        m.wait()


def solution(mesh):
    def device_fn(h_init, c_init, w_rec, gate_bias):
        hbm = pl.BlockSpec(memory_space=pl.ANY)
        vmem = pl.BlockSpec(memory_space=pltpu.VMEM)
        bf16, f32 = jnp.bfloat16, jnp.float32
        dma = pltpu.SemaphoreType.DMA
        tiles = (2, 6, 4, 3, S, CDIM)
        outs = (jax.ShapeDtypeStruct((STEPS,) + tiles, bf16), jax.ShapeDtypeStruct(tiles, f32))
        state = pl.pallas_call(
            kernel,
            out_shape=tuple(pltpu.VMEM(o.shape, o.dtype) for o in outs),
            in_specs=[hbm] * 4,
            out_specs=(vmem, vmem),
            scratch_shapes=[
                pltpu.VMEM(tiles, bf16),
                pltpu.VMEM(tiles, f32),
                pltpu.VMEM((CH, CH, 3, 3, LANES, 4 * LANES), bf16),
                pltpu.VMEM((4 * CH, STEPS, LANES), f32),
                pltpu.VMEM((CH, 8, 5, 16, LANES), bf16),
                pltpu.VMEM((CH, GROWS, LANES), f32),
                pltpu.VMEM((CH, GROWS, LANES), f32),
                pltpu.VMEM((CH, S * T * T, LANES), bf16),
                pltpu.VMEM((S * T * T // 2, 4 * LANES), f32),
                pltpu.VMEM((CH, S * T * T, LANES), f32),
                pltpu.VMEM((CH, RTILES * 16, LANES), f32),
                pltpu.VMEM((CH, TAPS, RTILES * 16, LANES), bf16),
                pltpu.VMEM((SLOTS, 2, 4, 3, S, CDIM), bf16),
                pltpu.VMEM((SLOTS, 2, 2, 6, S, CDIM), bf16),
                pltpu.VMEM((SLOTS, 4, 2, 2, S, CDIM), bf16),
                pltpu.VMEM((2, 4, 3, S, CDIM), bf16),
                pltpu.VMEM((2, 2, 6, S, CDIM), bf16),
                pltpu.VMEM((4, 1, 1, S, CDIM), bf16),
                pltpu.VMEM((2, 4, 3, S, CDIM), f32),
                pltpu.VMEM((2, 2, 6, S, CDIM), f32),
                pltpu.VMEM((4, 1, 1, S, CDIM), f32),
                dma((CH,)),
                dma,
                dma((2,)),
                dma((8,)),
                dma((SLOTS, 8)),
                dma((2, 8)),
                dma((2, 8)),
            ],
            compiler_params=pltpu.CompilerParams(
                collective_id=0, has_side_effects=True, vmem_limit_bytes=58 * 1024 * 1024
            ),
        )(
            h_init.transpose(1, 2, 0, 3).reshape(tiles),
            c_init.transpose(1, 2, 0, 3).reshape(tiles),
            w_rec,
            gate_bias,
        )
        h_seq, c_last = pl.pallas_call(
            copy_out,
            out_shape=outs,
            in_specs=[vmem] * 2,
            out_specs=(hbm, hbm),
            scratch_shapes=[dma((2,))],
            compiler_params=pltpu.CompilerParams(vmem_limit_bytes=16 * 1024 * 1024),
        )(*state)
        h_seq = h_seq.reshape(STEPS, T, T, S, CDIM).transpose(0, 3, 1, 2, 4)
        return h_seq, c_last.reshape(T, T, S, CDIM).transpose(2, 0, 1, 3)

    state_spec = P("dp", "rows", "cols", None)
    return jax.shard_map(
        device_fn,
        mesh=mesh,
        in_specs=(state_spec, state_spec, P(), P()),
        out_specs=(P(None, "dp", "rows", "cols", None), state_spec),
        check_vma=False,
    )
```

```python
import jax
import jax.numpy as jnp
from jax import lax
from jax.experimental import pallas as pl
from jax.experimental.pallas import tpu as pltpu
from jax.sharding import PartitionSpec as P

MESH = pl.DeviceIdType.MESH
STEPS = 12
S = 2
T = 12
LANES = 128
CH = 3
CDIM = CH * LANES
TAPS = 9
KDIM = TAPS * CDIM
SLOTS = 4

YPITCH = 3 * 6 * S
GROWS = 20 * YPITCH
RTILES = 7
ALL = ((0, 6, 0, 3),)
FIRST, SECOND = ((0, 3, 0, 3),), ((3, 6, 0, 3),)
INNER = ((1, 5, 1, 2),)
OUTER = ((0, 6, 0, 1), (0, 6, 2, 3), (0, 1, 1, 2), (5, 6, 1, 2))

DIRS = ((-1, 0), (1, 0), (0, -1), (0, 1), (-1, -1), (-1, 1), (1, -1), (1, 1))


def opposite(d):
    dy, dx = DIRS[d]
    return DIRS.index((-dy, -dx))


def at(y, x):
    return ((y + 2) * 3 + (x + 2) % 3) * 6 * S + (x + 2) // 3 * S


def sigmoid(v):
    return 0.5 * jnp.tanh(0.5 * v) + 0.5


def lstm(gates, bias, c_prev):
    i, f, o, g = (gates[:, k * LANES : (k + 1) * LANES] + bias[k] for k in range(4))
    c = sigmoid(f) * c_prev + sigmoid(i) * jnp.tanh(g)
    h = (sigmoid(o) * jnp.tanh(c)).astype(jnp.bfloat16)
    return h, c


def side_rows(dy):
    return -1 if dy < 0 else T


def ring_rows(g, dy, dx):
    sub = lax.broadcasted_iota(jnp.int32, (8, LANES), 0)
    out = []
    for ix in range(3):
        for y in (-1, T):
            out.append(g[pl.ds(at(y + dy, ix + dx), 8), :])
    for x in (-1, T):
        for s in range(S):
            out.append(g[pl.ds(at(dy, x + dx) + s, 8, stride=YPITCH), :])
    for x in (-1, T):
        a = g[pl.ds(at(8 + dy, x + dx), 8, stride=YPITCH), :]
        b = g[pl.ds(at(4 + dy, x + dx) + 1, 8, stride=YPITCH), :]
        out.append(jnp.where(sub < 4, a, b))
    v = None
    for k, (y, x) in enumerate(((-1, -1), (-1, T), (T, -1), (T, T))):
        a = g[pl.ds(at(y + dy, x + dx) - 2 * k, 8), :]
        v = a if v is None else jnp.where(sub < 2 * k, v, a)
    return out + [v, v]


def put_ring(g, v):
    k = 0
    for ix in range(3):
        for y in (-1, T):
            g[pl.ds(at(y, ix), 8), :] = v[k]
            k += 1
    for x in (-1, T):
        for s in range(S):
            g[pl.ds(at(0, x) + s, 8, stride=YPITCH), :] = v[k]
            k += 1
    for x in (-1, T):
        for s in range(S):
            g[pl.ds(at(8, x) + s, 4, stride=YPITCH), :] = v[k][4 * s : 4 * s + 4]
        k += 1
    for j, (y, x) in enumerate(((-1, -1), (-1, T), (T, -1), (T, T))):
        g[pl.ds(at(y, x), 2), :] = v[k][2 * j : 2 * j + 2]


def lanes(c):
    return slice(c * LANES, (c + 1) * LANES)


def line_pieces(line, c):
    if line.shape[0] == 4:
        return [line[:, ix, :, lanes(c)].reshape(8, LANES) for ix in range(3)]
    return [line[jy, :, :, lanes(c)].reshape(12, LANES) for jy in range(2)]


def put_line(g, d, dist, pieces):
    dy, dx = DIRS[d]
    if dx == 0:
        y = -dist if dy < 0 else T - 1 + dist
        for ix in range(3):
            g[pl.ds(at(y, ix), 8), :] = pieces[ix]
    else:
        x = -dist if dx < 0 else T - 1 + dist
        for jy in range(2):
            for iy in range(6):
                g[pl.ds(at(6 * jy + iy, x), 2), :] = pieces[jy][2 * iy : 2 * iy + 2]


def put_cells(ref, c, v):
    k = 0
    for iy in range(6):
        for ix in range(3):
            for jy in range(2):
                ref[jy, iy, :, ix, :, lanes(c)] = v[k : k + 8].reshape(4, S, LANES)
                k += 8


def get_cells(ref, c):
    return jnp.concatenate(
        [
            ref[jy, iy, :, ix, :, lanes(c)].reshape(8, LANES)
            for iy in range(6)
            for ix in range(3)
            for jy in range(2)
        ],
        axis=0,
    )


def kernel(
    h_hbm, c_hbm, w_hbm, bias_hbm, h_seq, c_last,
    h_init, c_init, w, bias, pt, grid, cgrid, h_new, half, c_own, c_ring, lhs_ring,
    recv_v, recv_h, recv_k, first_v, first_h, first_k, firstc_v, firstc_h, firstc_k,
    w_sem, bias_sem, in_sem, send_sem, recv_sem, fsend_sem, frecv_sem,
):
    rows_n, cols_n = lax.axis_size("rows"), lax.axis_size("cols")
    my_row, my_col = lax.axis_index("rows"), lax.axis_index("cols")
    f32, bf16 = jnp.float32, jnp.bfloat16

    def lacks(d):
        dy, dx = DIRS[d]
        r = jnp.bool_(False) if dy == 0 else my_row == (0 if dy < 0 else rows_n - 1)
        c = jnp.bool_(False) if dx == 0 else my_col == (0 if dx < 0 else cols_n - 1)
        return r, c, jnp.logical_or(r, c)

    def flip(v):
        return v + 1 - 2 * lax.rem(v, 2)

    def peer(d, back):
        dy, dx = DIRS[d]
        lr, lc, lack = lacks(d)
        if dx == 0:
            r, c = my_row, flip(my_col)
        elif dy == 0:
            r, c = flip(my_row), my_col
        else:
            a = my_row if dy < 0 else rows_n - 1 - my_row
            b = my_col if dx < 0 else cols_n - 1 - my_col
            on_c = jnp.logical_and(lc, a >= 2)
            on_r = jnp.logical_and(lr, b >= 2)
            if back:
                a3, b3 = jnp.where(a == 1, 0, jnp.where(b == 1, 0, 1)), jnp.where(a == 1, 1, 0)
            else:
                a3, b3 = jnp.where(b == 1, 1, 0), jnp.where(jnp.logical_and(a == 0, b == 0), 1, 0)
            a2 = jnp.where(on_c, flip(a), jnp.where(on_r, 0, a3))
            b2 = jnp.where(on_c, 0, jnp.where(on_r, flip(b), b3))
            r = a2 if dy < 0 else rows_n - 1 - a2
            c = b2 if dx < 0 else cols_n - 1 - b2
        return {"rows": jnp.where(lack, r, my_row + dy), "cols": jnp.where(lack, c, my_col + dx)}

    lack = [lacks(d)[2] for d in range(8)]
    peers = [peer(d, False) for d in range(8)]
    landing = [jnp.where(lack[d], d, opposite(d)) for d in range(8)]

    def kept(d, v):
        return jnp.where(lack[d], jnp.zeros_like(v), v)

    def edge_cells(d, depth):
        dy, dx = DIRS[d]
        every = slice(None)
        if dx == 0:
            return (0, depth, every, every) if dy < 0 else (1, 5 - depth, every, every)
        return (every, every, 0, depth) if dx < 0 else (every, every, 3, 2 - depth)

    def corner_cells(d, n):
        dy, dx = DIRS[d]
        jy, iy = (0, slice(0, n)) if dy < 0 else (1, slice(6 - n, 6))
        jx, ix = (0, slice(0, n)) if dx < 0 else (3, slice(3 - n, 3))
        return jy, iy, jx, ix

    def remote(d, src, dst, dst_back, ssem, rsem, rsem_back, sending):
        return pltpu.make_async_remote_copy(
            src_ref=src, dst_ref=dst if sending else dst_back,
            send_sem=ssem, recv_sem=rsem if sending else rsem_back,
            device_id=peers[d], device_id_type=MESH,
        )

    def message(d, slot, sending, h):
        e = landing[d]
        if d < 2:
            src, dst = h.at[edge_cells(d, 1)], lambda k: recv_v.at[slot, k]
        elif d < 4:
            src, dst = h.at[edge_cells(d, 1)], lambda k: recv_h.at[slot, k - 2]
        else:
            src, dst = h.at[corner_cells(d, 2)], lambda k: recv_k.at[slot, k - 4]
        return remote(
            d, src, dst(e), dst(d), send_sem.at[d], recv_sem.at[slot, e], recv_sem.at[slot, d], sending
        )

    def first_message(d, k, sending):
        e = landing[d]
        cells = edge_cells(d, 0) if d < 4 else corner_cells(d, 1)
        src = (c_init if k else h_init).at[cells]
        if d < 2:
            dst = lambda j: (firstc_v if k else first_v).at[j]
        elif d < 4:
            dst = lambda j: (firstc_h if k else first_h).at[j - 2]
        else:
            dst = lambda j: (firstc_k if k else first_k).at[j - 4]
        return remote(
            d, src, dst(e), dst(d), fsend_sem.at[k, d], frecv_sem.at[k, e], frecv_sem.at[k, d], sending
        )

    h_in = pltpu.make_async_copy(h_hbm, h_init, in_sem.at[0])
    c_in = pltpu.make_async_copy(c_hbm, c_init, in_sem.at[1])
    h_in.start()
    c_in.start()
    barrier = pltpu.get_barrier_semaphore()
    for d in range(8):
        pl.semaphore_signal(barrier, inc=1, device_id=peer(d, True), device_id_type=MESH)

    bias_copies = [
        pltpu.make_async_copy(bias_hbm.at[:, pl.ds(k * LANES, LANES)], bias.at[k], bias_sem) for k in range(4 * CH)
    ]
    for m in bias_copies:
        m.start()
    for c in range(CH):
        for kc in range(CH):
            for g in range(4):
                pltpu.make_async_copy(
                    w_hbm.at[:, :, pl.ds(kc * LANES, LANES), pl.ds(g * CDIM + c * LANES, LANES)],
                    w.at[c, kc, :, :, :, pl.ds(g * LANES, LANES)],
                    w_sem.at[c],
                ).start()

    def w_wait(c):
        pltpu.make_async_copy(w.at[c], w.at[c], w_sem.at[c]).wait()

    h_in.wait()
    pl.semaphore_wait(barrier, 8)
    for d in range(8):
        first_message(d, 0, True).start()
    for d in range(8):
        message(d, 0, True, h_init).start()
    c_in.wait()
    for d in range(8):
        first_message(d, 1, True).start()
    for c in range(CH):
        c_own[c] = get_cells(c_init, c).reshape(6, 3, 16, LANES)

    def put_own(g, hf):
        k = 0
        for iy in range(6):
            for ix in range(3):
                for jy in range(2):
                    g[pl.ds(at(6 * jy + iy, ix), 8), :] = hf[k : k + 8]
                    k += 8

    for c in range(CH):
        h = get_cells(h_init, c)
        pt[c, 1:7, 1:4] = h.reshape(6, 3, 16, LANES)
        put_own(grid.at[c], h.astype(f32))

    def take_first(k, to, gv, gh, gk):
        for d in range(8):
            first_message(d, k, False).wait_recv()
        for c in range(CH):
            g = to.at[c]
            for d in range(4):
                v = line_pieces((gv if d < 2 else gh).at[d % 2], c)
                put_line(g, d, 1, [kept(d, a.astype(f32)) for a in v])
            for d in range(4, 8):
                v = gk[d - 4, 0, 0, :, lanes(c)].astype(f32)
                dy, dx = DIRS[d]
                g[pl.ds(at(side_rows(dy), side_rows(dx)), 2), :] = kept(d, v)

    def build_border(c):
        g = grid.at[c]
        for ty in range(-1, 7):
            for tx in range(-1, 4):
                if not (0 <= ty < 6 and 0 <= tx < 3):
                    v = jnp.concatenate([g[pl.ds(at(ty + 6 * jy, tx), 8), :] for jy in range(2)], axis=0)
                    pt[c, ty + 1, tx + 1] = v.astype(bf16)

    for m in bias_copies:
        m.wait()

    def bias_of(t, c):
        return [bias[g * CH + c, pl.ds(t, 1), :] for g in range(4)]

    def own_gates(c, blocks):
        parts = [
            jnp.concatenate(
                [
                    pt[kc, y0 + tap // 3 : y1 + tap // 3, x0 + tap % 3 : x1 + tap % 3].reshape(-1, LANES)
                    for y0, y1, x0, x1 in blocks
                ],
                axis=0,
            )
            for kc in range(CH)
            for tap in range(TAPS)
        ]
        return jnp.dot(
            jnp.concatenate(parts, axis=1), w[c].reshape(KDIM, 4 * LANES), preferred_element_type=f32
        )

    def own_update(t, c, blocks, gates):
        row = 0
        for y0, y1, x0, x1 in blocks:
            shape = y1 - y0, x1 - x0, 16, LANES
            n = shape[0] * shape[1] * 16
            h, cn = lstm(gates[row : row + n], bias_of(t, c), c_own[c, y0:y1, x0:x1].reshape(n, LANES))
            c_own[c, y0:y1, x0:x1] = cn.reshape(shape)
            h_new[c, y0:y1, x0:x1] = h.reshape(shape)
            row += n

    def new_rows(c):
        return h_new[c].reshape(S * T * T, LANES)

    def take(slot):
        for d in range(8):
            message(d, slot, False, h_init).wait_recv()
        for c in range(CH):
            g = grid.at[c]
            for d in range(4):
                v = line_pieces((recv_v if d < 2 else recv_h).at[slot, d % 2], c)
                put_line(g, d, 2, [kept(d, a.astype(f32)) for a in v])
            for d in range(4, 8):
                v = kept(d, recv_k[slot, d - 4, :, :, :, lanes(c)].reshape(8, LANES).astype(f32))
                dy, dx = DIRS[d]
                y0, x0 = (-2 if dy < 0 else T), (-2 if dx < 0 else T)
                for k in range(4):
                    y, x = y0 + k // 2, x0 + k % 2
                    if (y, x) != (side_rows(dy), side_rows(dx)):
                        g[pl.ds(at(y, x), 2), :] = v[2 * k : 2 * k + 2]

    def ring_mask():
        sub = lax.broadcasted_iota(jnp.int32, (8, LANES), 0)
        ok = [jnp.where(lack[d], 0.0, 1.0).astype(f32) for d in range(8)]
        full = lambda v: jnp.full((8, LANES), v, f32)
        out = [full(ok[0]), full(ok[1])] * 3 + [full(ok[2])] * 2 + [full(ok[3])] * 2 + [full(ok[2]), full(ok[3])]
        k = full(ok[7])
        for j in (2, 1, 0):
            k = jnp.where(sub < 2 * (j + 1), full(ok[4 + j]), k)
        return out + [k]

    def ring(t, between):
        mask = ring_mask()
        for c in range(CH):
            parts = [lhs_ring[kc, tap] for kc in range(CH) for tap in range(TAPS)]
            gates = jnp.dot(
                jnp.concatenate(parts, axis=1), w[c].reshape(KDIM, 4 * LANES), preferred_element_type=f32
            )
            if c == 0:
                between()
            h, cn = lstm(gates, bias_of(t, c), c_ring[c])
            c_ring[c] = cn
            hf = h.astype(f32)
            put_ring(grid.at[c], [hf[8 * k : 8 * k + 8] * m for k, m in enumerate(mask)])
            build_border(c)

    def put_new(t):
        for c in range(CH):
            h = new_rows(c)
            put_cells(h_seq.at[t], c, h)
            pt[c, 1:7, 1:4] = h.reshape(6, 3, 16, LANES)

    def begin(t, blocks=ALL):
        for c in range(2):
            own_update(t, c, blocks, own_gates(c, blocks))
        half[...] = own_gates(2, FIRST)

    def finish(t):
        own_update(t, 2, FIRST, half[...])
        own_update(t, 2, SECOND, own_gates(2, SECOND))
        put_new(t)

    def sent(slot):
        for d in range(8):
            message(d, slot, True, h_init).wait_send()

    def step(t, carry):
        sent(lax.rem(t, SLOTS))
        take(lax.rem(t, SLOTS))
        for kc in range(CH):
            for tap in range(TAPS):
                v = ring_rows(grid.at[kc], tap // 3 - 1, tap % 3 - 1)
                lhs_ring[kc, tap] = jnp.concatenate(v, axis=0).astype(bf16)
        finish(t)

        def send():
            for d in (4, 5, 6, 7, 2, 3, 0, 1):
                message(d, lax.rem(t + 1, SLOTS), True, h_seq.at[t]).start()
            for c in range(CH):
                put_own(grid.at[c], new_rows(c).astype(f32))

        ring(t, send)
        begin(t + 1)
        return carry

    for c in range(2):
        w_wait(c)
        own_update(0, c, INNER, own_gates(c, INNER))
    take_first(0, grid, first_v, first_h, first_k)
    for d in range(8):
        first_message(d, 0, False).wait_send()
    for c in range(CH):
        build_border(c)
    w_wait(2)
    begin(0, OUTER)
    for d in range(8):
        first_message(d, 1, False).wait_send()
    take_first(1, cgrid, firstc_v, firstc_h, firstc_k)
    for c in range(CH):
        c_ring[c] = jnp.concatenate(ring_rows(cgrid.at[c], 0, 0), axis=0)

    lax.fori_loop(0, STEPS - 1, step, 0)
    sent((STEPS - 1) % SLOTS)
    for d in range(8):
        message(d, (STEPS - 1) % SLOTS, False, h_init).wait_recv()
    finish(STEPS - 1)
    for c in range(CH):
        put_cells(c_last, c, c_own[c].reshape(S * T * T, LANES))


def copy_out(h, c, h_out, c_out, sem):
    copies = [pltpu.make_async_copy(h, h_out, sem.at[0]), pltpu.make_async_copy(c, c_out, sem.at[1])]
    for m in copies:
        m.start()
    for m in copies:
        m.wait()


def solution(mesh):
    def device_fn(h_init, c_init, w_rec, gate_bias):
        hbm = pl.BlockSpec(memory_space=pl.ANY)
        vmem = pl.BlockSpec(memory_space=pltpu.VMEM)
        bf16, f32 = jnp.bfloat16, jnp.float32
        dma = pltpu.SemaphoreType.DMA
        tiles = (2, 6, 4, 3, S, CDIM)
        outs = (jax.ShapeDtypeStruct((STEPS,) + tiles, bf16), jax.ShapeDtypeStruct(tiles, f32))
        state = pl.pallas_call(
            kernel,
            out_shape=tuple(pltpu.VMEM(o.shape, o.dtype) for o in outs),
            in_specs=[hbm] * 4,
            out_specs=(vmem, vmem),
            scratch_shapes=[
                pltpu.VMEM(tiles, bf16),
                pltpu.VMEM(tiles, f32),
                pltpu.VMEM((CH, CH, 3, 3, LANES, 4 * LANES), bf16),
                pltpu.VMEM((4 * CH, STEPS, LANES), f32),
                pltpu.VMEM((CH, 8, 5, 16, LANES), bf16),
                pltpu.VMEM((CH, GROWS, LANES), f32),
                pltpu.VMEM((CH, GROWS, LANES), f32),
                pltpu.VMEM((CH, 6, 3, 16, LANES), bf16),
                pltpu.VMEM((S * T * T // 2, 4 * LANES), f32),
                pltpu.VMEM((CH, 6, 3, 16, LANES), f32),
                pltpu.VMEM((CH, RTILES * 16, LANES), f32),
                pltpu.VMEM((CH, TAPS, RTILES * 16, LANES), bf16),
                pltpu.VMEM((SLOTS, 2, 4, 3, S, CDIM), bf16),
                pltpu.VMEM((SLOTS, 2, 2, 6, S, CDIM), bf16),
                pltpu.VMEM((SLOTS, 4, 2, 2, S, CDIM), bf16),
                pltpu.VMEM((2, 4, 3, S, CDIM), bf16),
                pltpu.VMEM((2, 2, 6, S, CDIM), bf16),
                pltpu.VMEM((4, 1, 1, S, CDIM), bf16),
                pltpu.VMEM((2, 4, 3, S, CDIM), f32),
                pltpu.VMEM((2, 2, 6, S, CDIM), f32),
                pltpu.VMEM((4, 1, 1, S, CDIM), f32),
                dma((CH,)),
                dma,
                dma((2,)),
                dma((8,)),
                dma((SLOTS, 8)),
                dma((2, 8)),
                dma((2, 8)),
            ],
            compiler_params=pltpu.CompilerParams(
                collective_id=0, has_side_effects=True, vmem_limit_bytes=58 * 1024 * 1024
            ),
        )(
            h_init.transpose(1, 2, 0, 3).reshape(tiles),
            c_init.transpose(1, 2, 0, 3).reshape(tiles),
            w_rec,
            gate_bias,
        )
        h_seq, c_last = pl.pallas_call(
            copy_out,
            out_shape=outs,
            in_specs=[vmem] * 2,
            out_specs=(hbm, hbm),
            scratch_shapes=[dma((2,))],
            compiler_params=pltpu.CompilerParams(vmem_limit_bytes=16 * 1024 * 1024),
        )(*state)
        h_seq = h_seq.reshape(STEPS, T, T, S, CDIM).transpose(0, 3, 1, 2, 4)
        return h_seq, c_last.reshape(T, T, S, CDIM).transpose(2, 0, 1, 3)

    state_spec = P("dp", "rows", "cols", None)
    return jax.shard_map(
        device_fn,
        mesh=mesh,
        in_specs=(state_spec, state_spec, P(), P()),
        out_specs=(P(None, "dp", "rows", "cols", None), state_spec),
        check_vma=False,
    )
```

```python
import jax
import jax.numpy as jnp
from jax import lax
from jax.experimental import pallas as pl
from jax.experimental.pallas import tpu as pltpu
from jax.sharding import PartitionSpec as P

MESH = pl.DeviceIdType.MESH
STEPS = 12
S = 2
T = 12
LANES = 128
CH = 3
CDIM = CH * LANES
TAPS = 9
KDIM = TAPS * CDIM
SLOTS = 4

YPITCH = 3 * 6 * S
GROWS = 20 * YPITCH
RTILES = 7
ALL = ((0, 6, 0, 3),)
FIRST, SECOND = ((0, 3, 0, 3),), ((3, 6, 0, 3),)
INNER = ((1, 5, 1, 2),)
OUTER = ((0, 6, 0, 1), (0, 6, 2, 3), (0, 1, 1, 2), (5, 6, 1, 2))

DIRS = ((-1, 0), (1, 0), (0, -1), (0, 1), (-1, -1), (-1, 1), (1, -1), (1, 1))


def opposite(d):
    dy, dx = DIRS[d]
    return DIRS.index((-dy, -dx))


def at(y, x):
    return ((y + 2) * 3 + (x + 2) % 3) * 6 * S + (x + 2) // 3 * S


def sigmoid(v):
    return 0.5 * jnp.tanh(0.5 * v) + 0.5


def lstm(gates, bias, c_prev):
    i, f, o, g = (gates[:, k * LANES : (k + 1) * LANES] + bias[k] for k in range(4))
    c = sigmoid(f) * c_prev + sigmoid(i) * jnp.tanh(g)
    h = (sigmoid(o) * jnp.tanh(c)).astype(jnp.bfloat16)
    return h, c


def side_rows(dy):
    return -1 if dy < 0 else T


def ring_rows(g, dy, dx):
    sub = lax.broadcasted_iota(jnp.int32, (8, LANES), 0)
    out = []
    for ix in range(3):
        for y in (-1, T):
            out.append(g[pl.ds(at(y + dy, ix + dx), 8), :])
    for x in (-1, T):
        for s in range(S):
            out.append(g[pl.ds(at(dy, x + dx) + s, 8, stride=YPITCH), :])
    for x in (-1, T):
        a = g[pl.ds(at(8 + dy, x + dx), 8, stride=YPITCH), :]
        b = g[pl.ds(at(4 + dy, x + dx) + 1, 8, stride=YPITCH), :]
        out.append(jnp.where(sub < 4, a, b))
    v = None
    for k, (y, x) in enumerate(((-1, -1), (-1, T), (T, -1), (T, T))):
        a = g[pl.ds(at(y + dy, x + dx) - 2 * k, 8), :]
        v = a if v is None else jnp.where(sub < 2 * k, v, a)
    return out + [v, v]


def put_ring(g, v):
    k = 0
    for ix in range(3):
        for y in (-1, T):
            g[pl.ds(at(y, ix), 8), :] = v[k]
            k += 1
    for x in (-1, T):
        for s in range(S):
            g[pl.ds(at(0, x) + s, 8, stride=YPITCH), :] = v[k]
            k += 1
    for x in (-1, T):
        for s in range(S):
            g[pl.ds(at(8, x) + s, 4, stride=YPITCH), :] = v[k][4 * s : 4 * s + 4]
        k += 1
    for j, (y, x) in enumerate(((-1, -1), (-1, T), (T, -1), (T, T))):
        g[pl.ds(at(y, x), 2), :] = v[k][2 * j : 2 * j + 2]


def lanes(c):
    return slice(c * LANES, (c + 1) * LANES)


def line_pieces(line, c):
    if line.shape[0] == 4:
        return [line[:, ix, :, lanes(c)].reshape(8, LANES) for ix in range(3)]
    return [line[jy, :, :, lanes(c)].reshape(12, LANES) for jy in range(2)]


def put_line(g, d, dist, pieces):
    dy, dx = DIRS[d]
    if dx == 0:
        y = -dist if dy < 0 else T - 1 + dist
        for ix in range(3):
            g[pl.ds(at(y, ix), 8), :] = pieces[ix]
    else:
        x = -dist if dx < 0 else T - 1 + dist
        for jy in range(2):
            for iy in range(6):
                g[pl.ds(at(6 * jy + iy, x), 2), :] = pieces[jy][2 * iy : 2 * iy + 2]


def put_cells(ref, c, v):
    k = 0
    for iy in range(6):
        for ix in range(3):
            for jy in range(2):
                ref[jy, iy, :, ix, :, lanes(c)] = v[k : k + 8].reshape(4, S, LANES)
                k += 8


def get_cells(ref, c):
    return jnp.concatenate(
        [
            ref[jy, iy, :, ix, :, lanes(c)].reshape(8, LANES)
            for iy in range(6)
            for ix in range(3)
            for jy in range(2)
        ],
        axis=0,
    )


def kernel(
    h_hbm, c_hbm, w_hbm, bias_hbm, h_seq, c_last,
    h_init, c_init, w, bias, pt, grid, cgrid, h_new, half, c_own, c_ring, lhs_ring,
    recv_v, recv_h, recv_k, first_v, first_h, first_k, firstc_v, firstc_h, firstc_k,
    w_sem, bias_sem, in_sem, send_sem, recv_sem, fsend_sem, frecv_sem,
):
    rows_n, cols_n = lax.axis_size("rows"), lax.axis_size("cols")
    my_row, my_col = lax.axis_index("rows"), lax.axis_index("cols")
    f32, bf16 = jnp.float32, jnp.bfloat16

    def lacks(d):
        dy, dx = DIRS[d]
        r = jnp.bool_(False) if dy == 0 else my_row == (0 if dy < 0 else rows_n - 1)
        c = jnp.bool_(False) if dx == 0 else my_col == (0 if dx < 0 else cols_n - 1)
        return r, c, jnp.logical_or(r, c)

    def flip(v):
        return v + 1 - 2 * lax.rem(v, 2)

    def peer(d, back):
        dy, dx = DIRS[d]
        lr, lc, lack = lacks(d)
        if dx == 0:
            r, c = my_row, flip(my_col)
        elif dy == 0:
            r, c = flip(my_row), my_col
        else:
            a = my_row if dy < 0 else rows_n - 1 - my_row
            b = my_col if dx < 0 else cols_n - 1 - my_col
            on_c = jnp.logical_and(lc, a >= 2)
            on_r = jnp.logical_and(lr, b >= 2)
            if back:
                a3, b3 = jnp.where(a == 1, 0, jnp.where(b == 1, 0, 1)), jnp.where(a == 1, 1, 0)
            else:
                a3, b3 = jnp.where(b == 1, 1, 0), jnp.where(jnp.logical_and(a == 0, b == 0), 1, 0)
            a2 = jnp.where(on_c, flip(a), jnp.where(on_r, 0, a3))
            b2 = jnp.where(on_c, 0, jnp.where(on_r, flip(b), b3))
            r = a2 if dy < 0 else rows_n - 1 - a2
            c = b2 if dx < 0 else cols_n - 1 - b2
        return {"rows": jnp.where(lack, r, my_row + dy), "cols": jnp.where(lack, c, my_col + dx)}

    lack = [lacks(d)[2] for d in range(8)]
    peers = [peer(d, False) for d in range(8)]
    landing = [jnp.where(lack[d], d, opposite(d)) for d in range(8)]

    def kept(d, v):
        return jnp.where(lack[d], jnp.zeros_like(v), v)

    def edge_cells(d, depth):
        dy, dx = DIRS[d]
        every = slice(None)
        if dx == 0:
            return (0, depth, every, every) if dy < 0 else (1, 5 - depth, every, every)
        return (every, every, 0, depth) if dx < 0 else (every, every, 3, 2 - depth)

    def corner_cells(d, n):
        dy, dx = DIRS[d]
        jy, iy = (0, slice(0, n)) if dy < 0 else (1, slice(6 - n, 6))
        jx, ix = (0, slice(0, n)) if dx < 0 else (3, slice(3 - n, 3))
        return jy, iy, jx, ix

    def remote(d, src, dst, dst_back, ssem, rsem, rsem_back, sending):
        return pltpu.make_async_remote_copy(
            src_ref=src, dst_ref=dst if sending else dst_back,
            send_sem=ssem, recv_sem=rsem if sending else rsem_back,
            device_id=peers[d], device_id_type=MESH,
        )

    def message(d, slot, sending, h):
        e = landing[d]
        if d < 2:
            src, dst = h.at[edge_cells(d, 1)], lambda k: recv_v.at[slot, k]
        elif d < 4:
            src, dst = h.at[edge_cells(d, 1)], lambda k: recv_h.at[slot, k - 2]
        else:
            src, dst = h.at[corner_cells(d, 2)], lambda k: recv_k.at[slot, k - 4]
        return remote(
            d, src, dst(e), dst(d), send_sem.at[d], recv_sem.at[slot, e], recv_sem.at[slot, d], sending
        )

    def first_message(d, k, sending):
        e = landing[d]
        cells = edge_cells(d, 0) if d < 4 else corner_cells(d, 1)
        src = (c_init if k else h_init).at[cells]
        if d < 2:
            dst = lambda j: (firstc_v if k else first_v).at[j]
        elif d < 4:
            dst = lambda j: (firstc_h if k else first_h).at[j - 2]
        else:
            dst = lambda j: (firstc_k if k else first_k).at[j - 4]
        return remote(
            d, src, dst(e), dst(d), fsend_sem.at[k, d], frecv_sem.at[k, e], frecv_sem.at[k, d], sending
        )

    h_in = pltpu.make_async_copy(h_hbm, h_init, in_sem.at[0])
    c_in = pltpu.make_async_copy(c_hbm, c_init, in_sem.at[1])
    h_in.start()
    c_in.start()
    barrier = pltpu.get_barrier_semaphore()
    for d in range(8):
        pl.semaphore_signal(barrier, inc=1, device_id=peer(d, True), device_id_type=MESH)

    bias_copies = [
        pltpu.make_async_copy(bias_hbm.at[:, pl.ds(k * LANES, LANES)], bias.at[k], bias_sem) for k in range(4 * CH)
    ]
    for m in bias_copies:
        m.start()
    for c in range(CH):
        for kc in range(CH):
            for g in range(4):
                pltpu.make_async_copy(
                    w_hbm.at[:, :, pl.ds(kc * LANES, LANES), pl.ds(g * CDIM + c * LANES, LANES)],
                    w.at[c, kc, :, :, :, pl.ds(g * LANES, LANES)],
                    w_sem.at[c],
                ).start()

    def w_wait(c):
        pltpu.make_async_copy(w.at[c], w.at[c], w_sem.at[c]).wait()

    h_in.wait()
    pl.semaphore_wait(barrier, 8)
    for d in range(8):
        first_message(d, 0, True).start()
    for d in range(8):
        message(d, 0, True, h_init).start()
    c_in.wait()
    for d in range(8):
        first_message(d, 1, True).start()
    for c in range(CH):
        c_own[c] = get_cells(c_init, c).reshape(6, 3, 16, LANES)

    def put_own(g, hf):
        k = 0
        for iy in range(6):
            for ix in range(3):
                for jy in range(2):
                    g[pl.ds(at(6 * jy + iy, ix), 8), :] = hf[k : k + 8]
                    k += 8

    for c in range(CH):
        h = get_cells(h_init, c)
        pt[c, 1:7, 1:4] = h.reshape(6, 3, 16, LANES)
        put_own(grid.at[c], h.astype(f32))

    def take_first(k, to, gv, gh, gk):
        for d in range(8):
            first_message(d, k, False).wait_recv()
        for c in range(CH):
            g = to.at[c]
            for d in range(4):
                v = line_pieces((gv if d < 2 else gh).at[d % 2], c)
                put_line(g, d, 1, [kept(d, a.astype(f32)) for a in v])
            for d in range(4, 8):
                v = gk[d - 4, 0, 0, :, lanes(c)].astype(f32)
                dy, dx = DIRS[d]
                g[pl.ds(at(side_rows(dy), side_rows(dx)), 2), :] = kept(d, v)

    def build_border(c):
        g = grid.at[c]
        for ty in range(-1, 7):
            for tx in range(-1, 4):
                if not (0 <= ty < 6 and 0 <= tx < 3):
                    v = jnp.concatenate([g[pl.ds(at(ty + 6 * jy, tx), 8), :] for jy in range(2)], axis=0)
                    pt[c, ty + 1, tx + 1] = v.astype(bf16)

    for m in bias_copies:
        m.wait()

    def bias_of(t, c):
        return [bias[g * CH + c, pl.ds(t, 1), :] for g in range(4)]

    def own_gates(c, blocks):
        parts = [
            jnp.concatenate(
                [
                    pt[kc, y0 + tap // 3 : y1 + tap // 3, x0 + tap % 3 : x1 + tap % 3].reshape(-1, LANES)
                    for y0, y1, x0, x1 in blocks
                ],
                axis=0,
            )
            for kc in range(CH)
            for tap in range(TAPS)
        ]
        return jnp.dot(
            jnp.concatenate(parts, axis=1), w[c].reshape(KDIM, 4 * LANES), preferred_element_type=f32
        )

    def own_update(t, c, blocks, gates):
        row = 0
        for y0, y1, x0, x1 in blocks:
            shape = y1 - y0, x1 - x0, 16, LANES
            n = shape[0] * shape[1] * 16
            h, cn = lstm(gates[row : row + n], bias_of(t, c), c_own[c, y0:y1, x0:x1].reshape(n, LANES))
            c_own[c, y0:y1, x0:x1] = cn.reshape(shape)
            h_new[c, y0:y1, x0:x1] = h.reshape(shape)
            row += n

    def new_rows(c):
        return h_new[c].reshape(S * T * T, LANES)

    def take(slot):
        for d in range(8):
            message(d, slot, False, h_init).wait_recv()
        for c in range(CH):
            g = grid.at[c]
            for d in range(4):
                v = line_pieces((recv_v if d < 2 else recv_h).at[slot, d % 2], c)
                put_line(g, d, 2, [kept(d, a.astype(f32)) for a in v])
            for d in range(4, 8):
                v = kept(d, recv_k[slot, d - 4, :, :, :, lanes(c)].reshape(8, LANES).astype(f32))
                dy, dx = DIRS[d]
                y0, x0 = (-2 if dy < 0 else T), (-2 if dx < 0 else T)
                for k in range(4):
                    y, x = y0 + k // 2, x0 + k % 2
                    if (y, x) != (side_rows(dy), side_rows(dx)):
                        g[pl.ds(at(y, x), 2), :] = v[2 * k : 2 * k + 2]

    def ring_mask():
        sub = lax.broadcasted_iota(jnp.int32, (8, LANES), 0)
        ok = [jnp.where(lack[d], 0.0, 1.0).astype(f32) for d in range(8)]
        full = lambda v: jnp.full((8, LANES), v, f32)
        out = [full(ok[0]), full(ok[1])] * 3 + [full(ok[2])] * 2 + [full(ok[3])] * 2 + [full(ok[2]), full(ok[3])]
        k = full(ok[7])
        for j in (2, 1, 0):
            k = jnp.where(sub < 2 * (j + 1), full(ok[4 + j]), k)
        return out + [k]

    def ring(t, between):
        mask = ring_mask()
        for c in range(CH):
            parts = [lhs_ring[kc, tap] for kc in range(CH) for tap in range(TAPS)]
            gates = jnp.dot(
                jnp.concatenate(parts, axis=1), w[c].reshape(KDIM, 4 * LANES), preferred_element_type=f32
            )
            if c == 0:
                between()
            h, cn = lstm(gates, bias_of(t, c), c_ring[c])
            c_ring[c] = cn
            hf = h.astype(f32)
            put_ring(grid.at[c], [hf[8 * k : 8 * k + 8] * m for k, m in enumerate(mask)])
            build_border(c)

    def put_new(t):
        for c in range(CH):
            h = new_rows(c)
            put_cells(h_seq.at[t], c, h)
            pt[c, 1:7, 1:4] = h.reshape(6, 3, 16, LANES)

    def begin(t, blocks=ALL):
        for c in range(2):
            own_update(t, c, blocks, own_gates(c, blocks))
        half[...] = own_gates(2, FIRST)

    def finish(t):
        own_update(t, 2, FIRST, half[...])
        own_update(t, 2, SECOND, own_gates(2, SECOND))
        put_new(t)

    def all_sent():
        for d in range(8):
            cells = h_seq.at[(slice(None),) + (edge_cells(d, 1) if d < 4 else corner_cells(d, 2))]
            remote(d, cells, cells, cells, send_sem.at[d], recv_sem.at[0, d], recv_sem.at[0, d], True).wait_send()

    def step(t, carry):
        take(lax.rem(t, SLOTS))
        for kc in range(CH):
            for tap in range(TAPS):
                v = ring_rows(grid.at[kc], tap // 3 - 1, tap % 3 - 1)
                lhs_ring[kc, tap] = jnp.concatenate(v, axis=0).astype(bf16)
        finish(t)

        def send():
            for d in (4, 5, 6, 7, 2, 3, 0, 1):
                message(d, lax.rem(t + 1, SLOTS), True, h_seq.at[t]).start()
            for c in range(CH):
                put_own(grid.at[c], new_rows(c).astype(f32))

        ring(t, send)
        begin(t + 1)
        return carry

    for c in range(2):
        w_wait(c)
        own_update(0, c, INNER, own_gates(c, INNER))
    take_first(0, grid, first_v, first_h, first_k)
    for d in range(8):
        first_message(d, 0, False).wait_send()
    for c in range(CH):
        build_border(c)
    w_wait(2)
    begin(0, OUTER)
    for d in range(8):
        first_message(d, 1, False).wait_send()
    take_first(1, cgrid, firstc_v, firstc_h, firstc_k)
    for c in range(CH):
        c_ring[c] = jnp.concatenate(ring_rows(cgrid.at[c], 0, 0), axis=0)

    lax.fori_loop(0, STEPS - 1, step, 0)
    all_sent()
    for d in range(8):
        message(d, (STEPS - 1) % SLOTS, False, h_init).wait_recv()
    finish(STEPS - 1)
    for c in range(CH):
        put_cells(c_last, c, c_own[c].reshape(S * T * T, LANES))


def copy_out(h, c, h_out, c_out, sem):
    copies = [pltpu.make_async_copy(h, h_out, sem.at[0]), pltpu.make_async_copy(c, c_out, sem.at[1])]
    for m in copies:
        m.start()
    for m in copies:
        m.wait()


def solution(mesh):
    def device_fn(h_init, c_init, w_rec, gate_bias):
        hbm = pl.BlockSpec(memory_space=pl.ANY)
        vmem = pl.BlockSpec(memory_space=pltpu.VMEM)
        bf16, f32 = jnp.bfloat16, jnp.float32
        dma = pltpu.SemaphoreType.DMA
        tiles = (2, 6, 4, 3, S, CDIM)
        outs = (jax.ShapeDtypeStruct((STEPS,) + tiles, bf16), jax.ShapeDtypeStruct(tiles, f32))
        state = pl.pallas_call(
            kernel,
            out_shape=tuple(pltpu.VMEM(o.shape, o.dtype) for o in outs),
            in_specs=[hbm] * 4,
            out_specs=(vmem, vmem),
            scratch_shapes=[
                pltpu.VMEM(tiles, bf16),
                pltpu.VMEM(tiles, f32),
                pltpu.VMEM((CH, CH, 3, 3, LANES, 4 * LANES), bf16),
                pltpu.VMEM((4 * CH, STEPS, LANES), f32),
                pltpu.VMEM((CH, 8, 5, 16, LANES), bf16),
                pltpu.VMEM((CH, GROWS, LANES), f32),
                pltpu.VMEM((CH, GROWS, LANES), f32),
                pltpu.VMEM((CH, 6, 3, 16, LANES), bf16),
                pltpu.VMEM((S * T * T // 2, 4 * LANES), f32),
                pltpu.VMEM((CH, 6, 3, 16, LANES), f32),
                pltpu.VMEM((CH, RTILES * 16, LANES), f32),
                pltpu.VMEM((CH, TAPS, RTILES * 16, LANES), bf16),
                pltpu.VMEM((SLOTS, 2, 4, 3, S, CDIM), bf16),
                pltpu.VMEM((SLOTS, 2, 2, 6, S, CDIM), bf16),
                pltpu.VMEM((SLOTS, 4, 2, 2, S, CDIM), bf16),
                pltpu.VMEM((2, 4, 3, S, CDIM), bf16),
                pltpu.VMEM((2, 2, 6, S, CDIM), bf16),
                pltpu.VMEM((4, 1, 1, S, CDIM), bf16),
                pltpu.VMEM((2, 4, 3, S, CDIM), f32),
                pltpu.VMEM((2, 2, 6, S, CDIM), f32),
                pltpu.VMEM((4, 1, 1, S, CDIM), f32),
                dma((CH,)),
                dma,
                dma((2,)),
                dma((8,)),
                dma((SLOTS, 8)),
                dma((2, 8)),
                dma((2, 8)),
            ],
            compiler_params=pltpu.CompilerParams(
                collective_id=0,
                has_side_effects=True,
                vmem_limit_bytes=58 * 1024 * 1024,
            ),
        )(
            h_init.transpose(1, 2, 0, 3).reshape(tiles),
            c_init.transpose(1, 2, 0, 3).reshape(tiles),
            w_rec,
            gate_bias,
        )
        h_seq, c_last = pl.pallas_call(
            copy_out,
            out_shape=outs,
            in_specs=[vmem] * 2,
            out_specs=(hbm, hbm),
            scratch_shapes=[dma((2,))],
            compiler_params=pltpu.CompilerParams(vmem_limit_bytes=16 * 1024 * 1024),
        )(*state)
        h_seq = h_seq.reshape(STEPS, T, T, S, CDIM).transpose(0, 3, 1, 2, 4)
        return h_seq, c_last.reshape(T, T, S, CDIM).transpose(2, 0, 1, 3)

    state_spec = P("dp", "rows", "cols", None)
    return jax.shard_map(
        device_fn,
        mesh=mesh,
        in_specs=(state_spec, state_spec, P(), P()),
        out_specs=(P(None, "dp", "rows", "cols", None), state_spec),
        check_vma=False,
    )
```
